128 devices in a mesh: dp: 8 (over x, core), mp: 16 (over y, z).
Axes of the slice: x: 4, y: 4, z: 4, core: 2. Of those that a mesh axis runs over, the one named last changes fastest.
Arguments:
- tokens: bfloat16 [256, 8192], P('dp', 'mp'), may hold values from -6 to 6
- gate_up_weight: bfloat16 [2, 8192, 15360], P(None, 'mp', 'dp'), may hold values from -0.0625 to 0.0625
- down_weight: bfloat16 [15360, 8192], P('dp', 'mp'), may hold values from -0.046875 to 0.046875
- gate_up_input_factor: bfloat16 [2, 8192, 64], P(None, 'mp'), may hold values from -0.0625 to 0.0625
- gate_up_output_factor: bfloat16 [2, 64, 15360], P(None, None, 'dp'), may hold values from -0.046875 to 0.046875
- down_input_factor: bfloat16 [15360, 64], P('dp'), may hold values from -0.046875 to 0.046875
- down_output_factor: bfloat16 [64, 8192], P(None, 'mp'), may hold values from -0.0625 to 0.0625
- cotangent: bfloat16 [256, 8192], P('dp', 'mp'), may hold values from -6 to 6
Outputs:
- output: bfloat16 [256, 8192], P('dp', 'mp')
- input_grad: bfloat16 [256, 8192], P('dp', 'mp')
- grad_gate_up_lower: float32 [2, 8192, 64], P(None, 'mp')
- gate_up_output_factor_gradient: float32 [2, 64, 15360], P(None, None, 'dp')
- down_input_factor_gradient: float32 [15360, 64], P('dp')
- down_output_factor_gradient: float32 [64, 8192], P(None, 'mp')
The draws below stay inside these ranges and needn't reach their ends.
All inputs are finite; a program needn't handle non-finite values.
Results may differ from the reference program's by a relative error of at most 0.0065.
Values may be sent and summed in bfloat16 or wider, within the bound.
A program may use at most 64 MiB of HBM per device.

```python
import jax
import jax.numpy as jnp
from jax import lax

D = 8192
FF = 15360
R = 64
TOKENS = 256


def steps_of(key, dims, cuts, low, high):
    loudness = 1.0
    for dim, parts in cuts:
        draws = jax.random.uniform(jax.random.fold_in(jax.random.fold_in(key, 6), dim), (parts,), jnp.float32, low / len(cuts), high / len(cuts))
        loudness = loudness * jnp.repeat(jnp.exp(draws), dims[dim] // parts).reshape((-1,) + (1,) * (len(dims) - 1 - dim))
    return loudness


def normal_values(stream_key, shape, width, bound, split=(), dtype=jnp.bfloat16):
    gain = steps_of(stream_key, shape, split, -0.22, 0.18) if split else 1.0
    values = jax.random.normal(stream_key, shape, jnp.float32) * width * gain
    return jnp.minimum(jnp.maximum(values, -bound), bound).astype(dtype)


def setup_inputs(seed: int = 0) -> dict:
    key_of = jax.random.split(jax.random.key(seed), 9)
    tokens = normal_values(key_of[0], (TOKENS, D), 1.0, 6.0, ((0, 8), (1, 16)))
    gate_up_weight = normal_values(key_of[1], (2, D, FF), D ** -0.5, 0.0625, ((1, 16), (2, 8)))
    down_weight = normal_values(key_of[2], (FF, D), FF ** -0.5, 0.046875, ((0, 8), (1, 16)))
    gate_up_input_factor = normal_values(key_of[3], (2, D, R), D ** -0.5, 0.0625, ((1, 16),))
    gate_up_output_factor = normal_values(key_of[4], (2, R, FF), FF ** -0.5, 0.046875, ((2, 8),))
    down_input_factor = normal_values(key_of[5], (FF, R), FF ** -0.5, 0.046875, ((0, 8),))
    down_output_factor = normal_values(key_of[6], (R, D), D ** -0.5, 0.0625, ((1, 16),))
    cotangent = normal_values(key_of[7], (TOKENS, D), 1.0, 6.0, ((0, 8), (1, 16)))
    return {"tokens": tokens, "gate_up_weight": gate_up_weight, "down_weight": down_weight, "gate_up_input_factor": gate_up_input_factor, "gate_up_output_factor": gate_up_output_factor, "down_input_factor": down_input_factor, "down_output_factor": down_output_factor, "cotangent": cotangent}


adapter_scale = 2.0


def reference(tokens, gate_up_weight, down_weight, gate_up_input_factor, gate_up_output_factor, down_input_factor, down_output_factor, cotangent):
    single_float = jnp.float32
    upper_projection = lax.Precision.HIGHEST
    scale_factor = TOKENS ** -0.5
    lower_results = []
    pres = []
    for rank_dimension in range(2):
        lower_projection = jnp.dot(tokens, gate_up_input_factor[rank_dimension], preferred_element_type=single_float)
        lower_results.append(lower_projection)
        preactivation = jnp.dot(tokens, gate_up_weight[rank_dimension], preferred_element_type=single_float)
        preactivation = preactivation + adapter_scale * jnp.dot(lower_projection, gate_up_output_factor[rank_dimension].astype(single_float), precision=upper_projection)
        pres.append(preactivation)
    gate, upper = pres[0], pres[1]
    hidden_state = (jax.nn.silu(gate) * upper).astype(jnp.bfloat16)
    lower_down_projection = jnp.dot(hidden_state, down_input_factor, preferred_element_type=single_float)
    output = jnp.dot(hidden_state, down_weight, preferred_element_type=single_float)
    output = output + adapter_scale * jnp.dot(lower_down_projection, down_output_factor.astype(single_float), precision=upper_projection)
    output = output.astype(jnp.bfloat16)
    backward_down_rows = jnp.dot(cotangent, down_output_factor.T, preferred_element_type=single_float).astype(jnp.bfloat16)
    hidden_state_gradient = jnp.dot(cotangent, down_weight.T, preferred_element_type=single_float)
    hidden_state_gradient = hidden_state_gradient + adapter_scale * jnp.dot(backward_down_rows, down_input_factor.T, preferred_element_type=single_float)
    down_input_factor_gradient = adapter_scale * scale_factor * jnp.dot(hidden_state.T, backward_down_rows, preferred_element_type=single_float)
    down_output_factor_gradient = adapter_scale * scale_factor * jnp.dot(lower_down_projection.T, cotangent.astype(single_float), precision=upper_projection)
    sigma = jax.nn.sigmoid(gate)
    gate_back = (hidden_state_gradient * upper * sigma * (1.0 + gate * (1.0 - sigma))).astype(jnp.bfloat16)
    up_back = (hidden_state_gradient * gate * sigma).astype(jnp.bfloat16)
    backward_results = [gate_back, up_back]
    output_factor_gradient = []
    input_factor_gradient = []
    input_total_sum = jnp.zeros(tokens.shape, single_float)
    for rank_dimension in range(2):
        output_factor_gradient.append(adapter_scale * scale_factor * jnp.dot(lower_results[rank_dimension].T, backward_results[rank_dimension].astype(single_float), precision=upper_projection))
        backward_lower_rows = jnp.dot(backward_results[rank_dimension], gate_up_output_factor[rank_dimension].T, preferred_element_type=single_float).astype(jnp.bfloat16)
        input_factor_gradient.append(adapter_scale * scale_factor * jnp.dot(tokens.T, backward_lower_rows, preferred_element_type=single_float))
        input_total_sum = input_total_sum + jnp.dot(backward_results[rank_dimension], gate_up_weight[rank_dimension].T, preferred_element_type=single_float)
        input_total_sum = input_total_sum + adapter_scale * jnp.dot(backward_lower_rows, gate_up_input_factor[rank_dimension].T, preferred_element_type=single_float)
    input_grad = input_total_sum.astype(jnp.bfloat16)
    return (output, input_grad, jnp.stack(input_factor_gradient), jnp.stack(output_factor_gradient), down_input_factor_gradient, down_output_factor_gradient)
```

```python
import jax
import jax.numpy as jnp
from jax import lax
from jax.experimental import pallas as pl
from jax.experimental.pallas import tpu as pltpu
from jax.sharding import Mesh
from jax.sharding import PartitionSpec as P

MESH = pl.DeviceIdType.MESH
F32 = jnp.float32
BF16 = jnp.bfloat16

X, C, Y, Z = 4, 2, 4, 4
T = 256
DS = 512
FS = 1920
R = 64
EXT = 256
SCALE = 2.0 * T ** -0.5

SUBS = (
    ("y", 0, 512, False),
    ("z", 1024, 384, True),
    ("y", 512, 512, False),
    ("z", 1408, 512, False),
)
WIDTHS = tuple(3 * hw + (EXT if ext else 0) for _, _, hw, ext in SUBS)
NS = len(SUBS)
N_SEM = 48 + 24 * NS


def nn(a, b):
    return jnp.dot(a, b, preferred_element_type=F32)


def nt(a, b):
    return lax.dot_general(a, b, (((1,), (1,)), ((), ())), preferred_element_type=F32)


def body(tok, w_hbm, wd_hbm, at_hbm, b_hbm, dint_hbm, dout_hbm, cot,
         o_out, o_in, o_gl, o_gf, o_di, o_do,
         xc, w, wd, at, bf, dint, dout, acc_o, acc_i, acc_e, qt, rt, uq, rx, eg, *rest):
    per = len(rest) - 3
    each = per // NS
    bufs = [rest[s * each:(s + 1) * each] for s in range(NS)]
    local_sem, send_sem, recv_sem = rest[per:]
    me = {a: lax.axis_index(a) for a in ("x", "c", "y", "z")}

    def at_off(axis, off):
        return lax.rem(me[axis] + off, 4)

    count = [0]
    started = []

    def put(src, dst, device):
        n = count[0]
        count[0] += 1
        c = pltpu.make_async_remote_copy(
            src_ref=src, dst_ref=dst, send_sem=send_sem.at[n], recv_sem=recv_sem.at[n],
            device_id=device, device_id_type=MESH)
        c.start()
        started.append(c)
        return c

    other = 1 - me["c"]
    barrier = pltpu.get_barrier_semaphore()
    partners = [{"c": other}]
    for off in (1, 2, 3):
        partners += [{"x": at_off("x", off)}, {"x": at_off("x", off), "c": other},
                     {"y": at_off("y", off)}, {"z": at_off("z", off)}]
    for p in partners:
        pl.semaphore_signal(barrier, inc=1, device_id=p, device_id_type=MESH)

    my_dp = me["x"] * 2 + me["c"]
    loads = []
    for n, (src, dst) in enumerate((
        (tok, xc.at[0, my_dp]), (cot, xc.at[1, my_dp]), (at_hbm, at), (dout_hbm, dout),
        (b_hbm, bf), (dint_hbm, dint), (w_hbm, w), (wd_hbm, wd),
    )):
        c = pltpu.make_async_copy(src, dst, local_sem.at[n])
        c.start()
        loads.append(c)
    loads[0].wait()
    loads[1].wait()
    pl.semaphore_wait(barrier, len(partners))

    def block(off):
        return at_off("x", off) * 2 + me["c"]

    def whole(off):
        return xc.at[:, block(off)]

    g_right = put(whole(0), whole(0), {"x": at_off("x", 1)})
    g_left = put(whole(0), whole(0), {"x": at_off("x", 3)})
    g_pair = [put(whole(0), whole(0), {"c": other})]
    g_right.wait_recv()
    f_right = put(xc.at[0, block(3)], xc.at[0, block(3)], {"x": at_off("x", 1)})
    g_left.wait_recv()
    f_left = put(xc.at[1, block(1)], xc.at[1, block(1)], {"x": at_off("x", 3)})
    g_pair.append(put(whole(3), whole(3), {"c": other}))
    g_pair.append(put(whole(1), whole(1), {"c": other}))
    for c in loads[2:]:
        c.wait()
    f_right.wait_recv()
    f_left.wait_recv()
    g_pair.append(put(whole(2), whole(2), {"c": other}))
    for c in g_pair:
        c.wait_recv()

    xs = xc[0].reshape(T, DS)
    cs = xc[1].reshape(T, DS)
    low = [nt(xs, at[k]) for k in range(2)]
    bd = nt(cs, dout[...])
    low2 = [(2.0 * v).astype(BF16) for v in low]
    bd2 = (2.0 * bd).astype(BF16)

    def seg(n, hw):
        return slice(n * hw, (n + 1) * hw)

    def compute(s):
        _, f0, hw, ext = SUBS[s]
        p, q = bufs[s][0], bufs[s][1]
        cols = slice(f0, f0 + hw)
        for n in range(3):
            if n < 2:
                v = nn(xs, w[n, :, cols]) + nn(low2[n], bf[n, :, cols])
            else:
                v = nt(cs, wd[cols, :]) + nn(bd2, dint[:, cols])
            v = v.reshape(Y, Z, 16, hw)
            p[:, :, :, seg(n, hw)] = v
            q[:, :, :, seg(n, hw)] = v.astype(BF16)
        if ext:
            v = jnp.concatenate([low[0], low[1], bd, jnp.zeros_like(bd)], axis=1)
            v = v.reshape(Y, Z, 16, EXT)
            p[:, :, :, 3 * hw:] = v
            q[:, :, :, 3 * hw:] = v.astype(BF16)

    other_axis = {"y": "z", "z": "y"}

    def part(ref, s, a1, lo, hi):
        if SUBS[s][0] == "y":
            return ref.at[a1, lo:hi]
        return ref.at[lo:hi, a1]

    def value(ref, s, a1, a2):
        if SUBS[s][0] == "y":
            return ref[a1, a2]
        return ref[a2, a1]

    st = [dict() for _ in range(NS)]

    def rs1_send(s):
        a = SUBS[s][0]
        q, tr, tl, fr, fl = bufs[s][1], bufs[s][2], bufs[s][3], bufs[s][6], bufs[s][7]
        left, right = {a: at_off(a, 3)}, {a: at_off(a, 1)}
        st[s]["t"] = [
            put(part(q, s, at_off(a, 2), 0, 2), tr, left),
            put(part(q, s, at_off(a, 2), 2, 4), tl, right),
        ]
        st[s]["f"] = [
            put(part(q, s, at_off(a, 3), 2, 4), fr.at[2:4], left),
            put(part(q, s, at_off(a, 1), 0, 2), fl.at[0:2], right),
        ]

    def rs1_agg(s):
        a = SUBS[s][0]
        p, tr, tl, gr, gl, fr, fl = (bufs[s][k] for k in (0, 2, 3, 4, 5, 6, 7))
        left, right = {a: at_off(a, 3)}, {a: at_off(a, 1)}
        st[s]["t"][0].wait_recv()
        for j in range(2):
            gr[j] = (value(p, s, at_off(a, 3), j) + tr[j].astype(F32)).astype(BF16)
        st[s]["f"].append(put(gr, fr.at[0:2], left))
        st[s]["t"][1].wait_recv()
        for j in range(2):
            gl[j] = (value(p, s, at_off(a, 1), 2 + j) + tl[j].astype(F32)).astype(BF16)
        st[s]["f"].append(put(gl, fl.at[2:4], right))

    def rs1_fin(s):
        a = SUBS[s][0]
        b = other_axis[a]
        p, fr, fl, sm, q2, r2 = (bufs[s][k] for k in (0, 6, 7, 8, 9, 10))
        for c in st[s]["f"]:
            c.wait_recv()
        for j in range(4):
            v = value(p, s, me[a], j) + fr[j].astype(F32) + fl[j].astype(F32)
            sm[j] = v
            q2[j] = v.astype(BF16)
        st[s]["r"] = [
            put(q2.at[at_off(b, off)], r2.at[off - 1], {b: at_off(b, off)})
            for off in (2, 1, 3)
        ]

    def middle(s):
        a, f0, hw, ext = SUBS[s]
        b = other_axis[a]
        sm, r2, act = (bufs[s][k] for k in (8, 10, 11))
        for c in st[s]["r"]:
            c.wait_recv()

        def total(cols):
            v = sm[me[b], :, cols]
            for n in range(3):
                v = v + r2[n, :, cols].astype(F32)
            return v

        gate, up, hb = (total(seg(n, hw)) for n in range(3))
        sg = 1.0 / (1.0 + jnp.exp(-gate))
        my = (me["y"], me["z"])
        gs = gate * sg
        act[my[0], my[1], :, seg(0, hw)] = (gs * up).astype(BF16)
        act[my[0], my[1], :, seg(1, hw)] = (hb * up * sg * (1.0 + gate * (1.0 - sg))).astype(BF16)
        act[my[0], my[1], :, seg(2, hw)] = (hb * gs).astype(BF16)
        if ext:
            act[my[0], my[1], :, 3 * hw:] = total(slice(3 * hw, 3 * hw + EXT)).astype(BF16)
        mine = act.at[my[0], my[1]]
        st[s]["a1"] = [put(mine, mine, {b: at_off(b, off)}) for off in (2, 1, 3)]

    def ag2_send(s):
        a = SUBS[s][0]
        act = bufs[s][11]
        left, right = {a: at_off(a, 3)}, {a: at_off(a, 1)}
        for c in st[s]["a1"]:
            c.wait_recv()
        lo, hi = part(act, s, me[a], 0, 2), part(act, s, me[a], 2, 4)
        st[s]["fromright"] = [put(lo, lo, left)]
        st[s]["fromleft"] = [put(hi, hi, right)]
        st[s]["fromright"].append(put(hi, hi, left))
        st[s]["fromleft"].append(put(lo, lo, right))

    def ag2_fwd(s):
        a = SUBS[s][0]
        act = bufs[s][11]
        left, right = {a: at_off(a, 3)}, {a: at_off(a, 1)}
        st[s]["fromright"][0].wait_recv()
        src = part(act, s, at_off(a, 1), 0, 2)
        st[s]["fromright"].append(put(src, src, left))
        st[s]["fromleft"][0].wait_recv()
        src = part(act, s, at_off(a, 3), 2, 4)
        st[s]["fromleft"].append(put(src, src, right))

    def ag2_fin(s):
        for c in st[s]["fromright"][1:] + st[s]["fromleft"][1:]:
            c.wait_recv()

    def act_of(s, cols):
        n = cols.stop - cols.start
        return bufs[s][11][:, :, :, cols].reshape(T, n)

    first = [True]

    def post(s):
        _, f0, hw, ext = SUBS[s]
        cols = slice(f0, f0 + hw)
        hid, gb, ub = (act_of(s, seg(n, hw)) for n in range(3))
        o = nn(hid, wd[cols, :])
        i = nt(gb, w[0, :, cols]) + nt(ub, w[1, :, cols])
        e = [nt(gb, bf[0, :, cols]), nt(ub, bf[1, :, cols]), nt(hid, dint[:, cols])]
        if first[0]:
            acc_o[...] = o
            acc_i[...] = i
            for n in range(3):
                acc_e[n] = e[n]
            first[0] = False
        else:
            acc_o[...] += o
            acc_i[...] += i
            for n in range(3):
                acc_e[n] += e[n]

    def grads():
        s = [n for n in range(NS) if SUBS[n][3]][0]
        hw = SUBS[s][2]
        ext = act_of(s, slice(3 * hw, 3 * hw + EXT)).astype(F32)
        ext_t = jnp.transpose(ext).astype(BF16)
        for s in range(NS):
            _, f0, hw, _ = SUBS[s]
            cols = slice(f0, f0 + hw)
            for k in range(2):
                o_gf[k, :, cols] = SCALE * nn(ext_t[64 * k:64 * k + 64], act_of(s, seg(1 + k, hw)))
            o_di[:, cols] = SCALE * nn(ext_t[128:192], act_of(s, seg(0, hw)))

    order = range(NS)
    compute(0)
    rs1_send(0)
    compute(1)
    rs1_send(1)
    compute(2)
    compute(3)
    rs1_agg(0)
    rs1_agg(1)
    rs1_send(2)
    rs1_send(3)
    rs1_fin(0)
    rs1_fin(1)
    rs1_agg(2)
    rs1_agg(3)
    middle(0)
    middle(1)
    rs1_fin(2)
    rs1_fin(3)
    ag2_send(0)
    ag2_send(1)
    middle(2)
    middle(3)
    ag2_fwd(0)
    ag2_fwd(1)
    ag2_send(2)
    ag2_send(3)
    ag2_fin(0)
    post(0)
    ag2_fin(1)
    post(1)
    ag2_fwd(2)
    ag2_fwd(3)
    ag2_fin(2)
    post(2)
    ag2_fin(3)
    post(3)

    e2 = [(2.0 * acc_e[n]).astype(BF16) for n in range(3)]
    acc_o[...] += nn(e2[2], dout[...])
    acc_i[...] += nn(e2[0], at[0]) + nn(e2[1], at[1])
    tail = (slice(0, DS), slice(DS, 2 * DS), slice(2 * DS, 2 * DS + EXT))

    def rows_of(xi, c):
        return pl.ds(pl.multiple_of((xi * 2 + c) * 32, 32), 32)

    def mine_rows(xi, c):
        r = rows_of(xi, c)
        e = jnp.concatenate(
            [acc_e[0, r], acc_e[1, r], acc_e[2, r], jnp.zeros((32, R), F32)], axis=1)
        return acc_o[r, :], acc_i[r, :], e

    for xi in range(X):
        for cols, v in zip(tail, mine_rows(xi, other)):
            qt[xi, :, cols] = v.astype(BF16)
    pair = put(qt, rt, {"c": other})
    pair.wait_recv()
    xr = []
    for off in (2, 1, 3):
        xi = at_off("x", off)
        for cols, v in zip(tail, mine_rows(xi, me["c"])):
            uq[off - 1, :, cols] = (v + rt[xi, :, cols].astype(F32)).astype(BF16)
        xr.append(put(uq.at[off - 1], rx.at[off - 1], {"x": xi}))
    grads()
    own = [v + rt[me["x"], :, cols].astype(F32) for cols, v in zip(tail, mine_rows(me["x"], me["c"]))]
    for c in xr:
        c.wait_recv()
    res = []
    for cols, v in zip(tail, own):
        for n in range(3):
            v = v + rx[n, :, cols].astype(F32)
        res.append(v.astype(BF16))
    eg[my_dp] = res[2]
    mine = eg.at[my_dp]
    er = [put(mine, mine, {"c": other})]
    for off in (2, 1, 3):
        er.append(put(mine, mine, {"x": at_off("x", off)}))
        er.append(put(mine, mine, {"x": at_off("x", off), "c": other}))
    o_out[...] = res[0]
    o_in[...] = res[1]
    for c in er:
        c.wait_recv()
    e_t = jnp.transpose(eg[...].reshape(T, EXT).astype(F32)).astype(BF16)
    for k in range(2):
        o_gl[k] = SCALE * nn(e_t[64 * k:64 * k + 64], xc[0].reshape(T, DS))
    o_do[...] = SCALE * nn(e_t[128:192], xc[1].reshape(T, DS))
    for c in started:
        c.wait_send()


def per_device(tok, w, wd, a, b, din, dout, cot):
    at = jnp.swapaxes(a, 1, 2)
    dint = jnp.swapaxes(din, 0, 1)
    vm = pltpu.VMEM
    scratch = [
        vm((2, X * C, 32, DS), BF16), vm((2, DS, FS), BF16), vm((FS, DS), BF16),
        vm((2, R, DS), BF16), vm((2, R, FS), BF16), vm((R, FS), BF16), vm((R, DS), BF16),
        vm((T, DS), F32), vm((T, DS), F32), vm((3, T, R), F32),
        vm((X, 32, 2 * DS + EXT), BF16), vm((X, 32, 2 * DS + EXT), BF16),
        vm((3, 32, 2 * DS + EXT), BF16), vm((3, 32, 2 * DS + EXT), BF16),
        vm((X * C, 32, EXT), BF16),
    ]
    for wid in WIDTHS:
        scratch += [
            vm((Y, Z, 16, wid), F32), vm((Y, Z, 16, wid), BF16),
            vm((2, 16, wid), BF16), vm((2, 16, wid), BF16),
            vm((2, 16, wid), BF16), vm((2, 16, wid), BF16),
            vm((4, 16, wid), BF16), vm((4, 16, wid), BF16),
            vm((4, 16, wid), F32), vm((4, 16, wid), BF16), vm((3, 16, wid), BF16),
            vm((Y, Z, 16, wid), BF16),
        ]
    scratch += [pltpu.SemaphoreType.DMA((8,)), pltpu.SemaphoreType.DMA((N_SEM,)), pltpu.SemaphoreType.DMA((N_SEM,))]
    anyspec = pl.BlockSpec(memory_space=pl.ANY)
    vspec = pl.BlockSpec(memory_space=pltpu.VMEM)
    out, inp, gl, gf, di, do = pl.pallas_call(
        body,
        out_shape=(
            jax.ShapeDtypeStruct((32, DS), BF16), jax.ShapeDtypeStruct((32, DS), BF16),
            jax.ShapeDtypeStruct((2, R, DS), F32), jax.ShapeDtypeStruct((2, R, FS), F32),
            jax.ShapeDtypeStruct((R, FS), F32), jax.ShapeDtypeStruct((R, DS), F32),
        ),
        in_specs=[anyspec] * 8,
        out_specs=(vspec,) * 6,
        scratch_shapes=scratch,
        compiler_params=pltpu.CompilerParams(
            collective_id=0, has_side_effects=True, vmem_limit_bytes=60 * 1024 * 1024),
        name="layer",
    )(tok, w, wd, at, b, dint, dout, cot)
    return out, inp, jnp.swapaxes(gl, 1, 2), gf, jnp.swapaxes(di, 0, 1), do


def solution(mesh):
    torus = Mesh(mesh.devices.reshape(X, C, Y, Z), ("x", "c", "y", "z"))
    dp, mp = ("x", "c"), ("y", "z")
    in_specs = (
        P(dp, mp), P(None, mp, dp), P(dp, mp), P(None, mp, None),
        P(None, None, dp), P(dp, None), P(None, mp), P(dp, mp),
    )
    out_specs = (P(dp, mp), P(dp, mp), P(None, mp, None), P(None, None, dp), P(dp, None), P(None, mp))
    return jax.shard_map(per_device, mesh=torus, in_specs=in_specs, out_specs=out_specs, check_vma=False)
```

```python
import jax
import jax.numpy as jnp
from jax import lax
from jax.experimental import pallas as pl
from jax.experimental.pallas import tpu as pltpu
from jax.sharding import Mesh
from jax.sharding import PartitionSpec as P

MESH = pl.DeviceIdType.MESH
F32 = jnp.float32
BF16 = jnp.bfloat16

X, C, Y, Z = 4, 2, 4, 4
T = 256
DS = 512
FS = 1920
R = 64
EXT = 256
SCALE = 2.0 * T ** -0.5

SUBS = (
    ("z", 1024, 128, True), ("y", 0, 256, False), ("z", 1152, 256, False), ("y", 256, 256, False),
    ("z", 1408, 256, False), ("y", 512, 256, False), ("z", 1664, 256, False), ("y", 768, 256, False),
)
WIDTHS = tuple(3 * hw + (EXT if ext else 0) for _, _, hw, ext in SUBS)
NS = len(SUBS)
N_RECV = 11 + 8 * NS
N_SENT = 11 + NS


def steps_of(subs, *names):
    return [(name, s) for s in subs for name in names]


SCHEDULE = (
    steps_of(range(NS), "gu", "hb", "send")
    + steps_of(range(NS), "agg") + steps_of(range(NS), "sum") + steps_of(range(NS), "mid")
    + [("esend", 0)] + steps_of(range(4), "spread") + [("esum", 0)] + steps_of(range(4, NS), "spread")
    + steps_of(range(4), "fwd") + [("emore", 0)] + steps_of(range(4, NS), "fwd")
    + [("fin", 0), ("out", 0), ("in", 0), ("flip", 0), ("grad", 0)]
    + steps_of(range(1, 6), "fin", "out", "in", "grad") + [("efin", 0)]
    + steps_of((6,), "fin", "out", "in")
    + [("fin", 7), ("out", 7), ("pair", 0), ("in", 7), ("pair", 1), ("grad", 6), ("xsend", 0), ("xsend", 1),
       ("grad", 7), ("xfin", 0), ("xfin", 1)]
)


def nn(a, b):
    return jnp.dot(a, b, preferred_element_type=F32)


def nt(a, b):
    return lax.dot_general(a, b, (((1,), (1,)), ((), ())), preferred_element_type=F32)


def body(tok, w_hbm, wd_hbm, at_hbm, b_hbm, dint_hbm, dout_hbm, cot,
         o_out, o_in, o_gl, o_gf, o_di, o_do,
         xc, w, wd, aw, cw, ew, acc_o, acc_i, ext2, e_acc, ext_t, lora,
         qt, rt, uq, rx, e_out, e_in, e_n, eg, xn, bytes_ref, *rest):
    per = len(rest) - 3
    each = per // NS
    bufs = [rest[s * each:(s + 1) * each] for s in range(NS)]
    local_sem, send_sem, recv_sem = rest[per:]
    me = {a: lax.axis_index(a) for a in ("x", "c", "y", "z")}

    def at_off(axis, off):
        return lax.rem(me[axis] + off, 4)

    arrivals, departures = [], []

    def sends(like):
        departures.append(like)
        return len(departures) - 1

    def group(like, out=None):
        arrivals.append(like)
        return len(arrivals) - 1, sends(like) if out is None else out

    def put(g, src, dst, device):
        pltpu.make_async_remote_copy(
            src_ref=src, dst_ref=dst, send_sem=send_sem.at[g[1]], recv_sem=recv_sem.at[g[0]],
            device_id=device, device_id_type=MESH).start()

    def arrived(g):
        pltpu.make_async_copy(arrivals[g[0]], arrivals[g[0]], recv_sem.at[g[0]]).wait()

    def sent(n):
        pltpu.make_async_copy(departures[n], departures[n], send_sem.at[n]).wait()

    other = 1 - me["c"]
    barrier = pltpu.get_barrier_semaphore()
    partners = [{"c": other}]
    for off in (1, 2, 3):
        partners += [{"x": at_off("x", off)}, {"x": at_off("x", off), "c": other},
                     {"y": at_off("y", off)}, {"z": at_off("z", off)}]
    for p in partners:
        pl.semaphore_signal(barrier, inc=1, device_id=p, device_id_type=MESH)

    my_dp = me["x"] * 2 + me["c"]
    loads = []
    for n, (src, dst) in enumerate((
        (tok, xc.at[0, my_dp]), (cot, xc.at[1, my_dp]), (at_hbm, aw), (dout_hbm, cw.at[0:64]),
        (b_hbm.at[0], ew.at[0, 0:64]), (b_hbm.at[1], ew.at[1, 64:128]), (dint_hbm, ew.at[2, 0:64]),
        (w_hbm, w), (wd_hbm, wd),
    )):
        c = pltpu.make_async_copy(src, dst, local_sem.at[n])
        c.start()
        loads.append(c)
    cw[64:128, :] = jnp.zeros((64, DS), BF16)
    ew[0, 64:128, :] = jnp.zeros((64, FS), BF16)
    ew[1, 0:64, :] = jnp.zeros((64, FS), BF16)
    ew[2, 64:128, :] = jnp.zeros((64, FS), BF16)
    loads[0].wait()
    loads[1].wait()
    pl.semaphore_wait(barrier, len(partners))

    def block(n, off):
        return xc.at[n, at_off("x", off) * 2 + me["c"]]

    along = [group(xn.at[0:3]) for _ in range(2)]
    across = [group(xn) for _ in range(2)]
    for n in range(2):
        for off in (2, 1, 3):
            put(along[n], block(n, 0), block(n, 0), {"x": at_off("x", off)})
        put(across[n], block(n, 0), block(n, 0), {"c": other})
    for c in loads[2:]:
        c.wait()
    for n in range(2):
        arrived(along[n])
        for off in (1, 2, 3):
            put(across[n], block(n, off), block(n, off), {"c": other})

    arrived(across[0])
    xs = xc[0].reshape(T, DS)
    late = {}

    def seg(n, hw):
        return slice(n * hw, (n + 1) * hw)

    def keep(s, cols, v):
        v = v.reshape(Y, Z, 16, v.shape[-1])
        bufs[s][0][:, :, :, cols] = v
        bufs[s][1][:, :, :, cols] = v.astype(BF16)

    def compute_gu(s):
        _, f0, hw, _ = SUBS[s]
        cols = slice(f0, f0 + hw)
        for n in range(2):
            keep(s, seg(n, hw), nn(xs, w[n, :, cols]))

    def compute_hb(s):
        _, f0, hw, ext = SUBS[s]
        cols = slice(f0, f0 + hw)
        if not late:
            arrived(across[1])
            late["c"] = xc[1].reshape(T, DS)
        keep(s, seg(2, hw), nt(late["c"], wd[cols, :]))
        if ext:
            keep(s, slice(3 * hw, 3 * hw + 128), nt(xs, aw[...]))
            keep(s, slice(3 * hw + 128, 3 * hw + EXT), nt(late["c"], cw[...]))

    other_axis = {"y": "z", "z": "y"}

    def part(ref, s, a1, lo, hi):
        if SUBS[s][0] == "y":
            return ref.at[a1, lo:hi]
        return ref.at[lo:hi, a1]

    def value(ref, s, a1, a2):
        if SUBS[s][0] == "y":
            return ref[a1, a2]
        return ref[a2, a1]

    st = []
    for s in range(NS):
        tt, ff, r2 = bufs[s][2], bufs[s][4], bufs[s][7]
        o = sends(bytes_ref.at[:, :, 0:WIDTHS[s]])
        st.append({
            "t0": group(tt.at[0], o), "t1": group(tt.at[1], o), "f": group(ff, o), "r": group(r2, o),
            "a": group(r2, o), "b0": group(tt.at[0], o), "b1": group(tt.at[1], o), "b2": group(ff, o)})

    def ring(s):
        a = SUBS[s][0]
        return a, {a: at_off(a, 3)}, {a: at_off(a, 1)}

    def rs1_send(s):
        a, left, right = ring(s)
        q, tt, ff = bufs[s][1], bufs[s][2], bufs[s][4]
        put(st[s]["t0"], part(q, s, at_off(a, 2), 0, 2), tt.at[0], left)
        put(st[s]["t1"], part(q, s, at_off(a, 2), 2, 4), tt.at[1], right)
        put(st[s]["f"], part(q, s, at_off(a, 3), 2, 4), ff.at[0, 2:4], left)
        put(st[s]["f"], part(q, s, at_off(a, 1), 0, 2), ff.at[1, 0:2], right)

    def rs1_agg(s):
        a, left, right = ring(s)
        p, tt, gg, ff = bufs[s][0], bufs[s][2], bufs[s][3], bufs[s][4]
        arrived(st[s]["t0"])
        for j in range(2):
            gg[0, j] = (value(p, s, at_off(a, 3), j) + tt[0, j].astype(F32)).astype(BF16)
        put(st[s]["f"], gg.at[0], ff.at[0, 0:2], left)
        arrived(st[s]["t1"])
        for j in range(2):
            gg[1, j] = (value(p, s, at_off(a, 1), 2 + j) + tt[1, j].astype(F32)).astype(BF16)
        put(st[s]["f"], gg.at[1], ff.at[1, 2:4], right)

    def rs1_fin(s):
        a = SUBS[s][0]
        b = other_axis[a]
        p, ff, sm, q2, r2 = (bufs[s][k] for k in (0, 4, 5, 6, 7))
        arrived(st[s]["f"])
        for j in range(4):
            v = value(p, s, me[a], j) + ff[0, j].astype(F32) + ff[1, j].astype(F32)
            sm[j] = v
            q2[j] = v.astype(BF16)
        for off in (2, 1, 3):
            put(st[s]["r"], q2.at[at_off(b, off)], r2.at[off - 1], {b: at_off(b, off)})

    seen = set()

    def add(ref, key, v):
        if key in seen:
            v = v + ref[...]
        seen.add(key)
        ref[...] = v

    def middle(s):
        a, f0, hw, ext = SUBS[s]
        b = other_axis[a]
        sm, r2, act = (bufs[s][k] for k in (5, 7, 8))
        arrived(st[s]["r"])

        def total(cols):
            v = sm[me[b], :, cols]
            for n in range(3):
                v = v + r2[n, :, cols].astype(F32)
            return v

        my = (me["y"], me["z"])
        cols = slice(f0, f0 + hw)
        if ext:
            v = total(slice(3 * hw, 3 * hw + EXT)).astype(BF16)
            act[my[0], my[1], :, 3 * hw:] = v
            ext2[...] = 2.0 * v
        lows = (ext2[:, 0:128], ext2[:, 0:128], ext2[:, 128:256])
        gate, up, hb = (total(seg(n, hw)) + nn(lows[n], ew[n, :, cols]) for n in range(3))
        sg = 1.0 / (1.0 + jnp.exp(-gate))
        gs = gate * sg
        hid = (gs * up).astype(BF16)
        gb = (hb * up * sg * (1.0 + gate * (1.0 - sg))).astype(BF16)
        ub = (hb * gs).astype(BF16)
        act[my[0], my[1], :, seg(0, hw)] = hid
        act[my[0], my[1], :, seg(1, hw)] = gb
        act[my[0], my[1], :, seg(2, hw)] = ub
        mine = act.at[my[0], my[1]]
        for off in (2, 1, 3):
            put(st[s]["a"], mine, mine, {b: at_off(b, off)})
        add(e_acc.at[:, 0:128], "bl", nt(gb, ew[0, :, cols]) + nt(ub, ew[1, :, cols]))
        add(e_acc.at[:, 128:256], "ld", nt(hid, ew[2, :, cols]))

    def ag2_send(s):
        a, left, right = ring(s)
        act = bufs[s][8]
        arrived(st[s]["a"])
        lo, hi = part(act, s, me[a], 0, 2), part(act, s, me[a], 2, 4)
        put(st[s]["b0"], lo, lo, left)
        put(st[s]["b1"], hi, hi, right)
        put(st[s]["b2"], hi, hi, left)
        put(st[s]["b2"], lo, lo, right)

    def ag2_fwd(s):
        a, left, right = ring(s)
        act = bufs[s][8]
        arrived(st[s]["b0"])
        src = part(act, s, at_off(a, 1), 0, 2)
        put(st[s]["b2"], src, src, left)
        arrived(st[s]["b1"])
        src = part(act, s, at_off(a, 3), 2, 4)
        put(st[s]["b2"], src, src, right)

    def ag2_fin(s):
        arrived(st[s]["b2"])

    def act_of(s, cols):
        return bufs[s][8][:, :, :, cols].reshape(T, cols.stop - cols.start)

    def post_o(s):
        _, f0, hw, _ = SUBS[s]
        add(acc_o, "o", nn(act_of(s, seg(0, hw)), wd[f0:f0 + hw, :]))

    def post_i(s):
        _, f0, hw, _ = SUBS[s]
        cols = slice(f0, f0 + hw)
        add(acc_i, "i", nt(act_of(s, seg(1, hw)), w[0, :, cols]) + nt(act_of(s, seg(2, hw)), w[1, :, cols]))

    def flip(_):
        hw = SUBS[0][2]
        ext = act_of(0, slice(3 * hw, 3 * hw + EXT)).astype(F32)
        ext_t[...] = jnp.transpose(ext).astype(BF16)

    def grads(s):
        _, f0, hw, _ = SUBS[s]
        cols = slice(f0, f0 + hw)
        for k in range(2):
            o_gf[k, :, cols] = SCALE * nn(ext_t[64 * k:64 * k + 64, :], act_of(s, seg(1 + k, hw)))
        o_di[:, cols] = SCALE * nn(ext_t[128:192, :], act_of(s, seg(0, hw)))

    my_rows = (me["y"], me["z"])
    e_dp, e_z, e_y = group(e_in), group(e_n.at[0]), group(e_n)
    hops = [(off, d) for off in (2, 1, 3, 0) for d in (0, 1) if off or d]

    def e_send(_):
        e_out[...] = e_acc[...].astype(BF16)
        for n, (off, d) in enumerate(hops):
            put(e_dp, e_out, e_in.at[n], {"x": at_off("x", off), "c": lax.rem(me["c"] + d, 2)})

    def e_sum(_):
        arrived(e_dp)
        v = e_acc[...]
        for n in range(7):
            v = v + e_in[n].astype(F32)
        eg[my_rows[0], my_rows[1]] = v.astype(BF16)
        mine = eg.at[my_rows[0], my_rows[1]]
        for off in (2, 1, 3):
            put(e_z, mine, mine, {"z": at_off("z", off)})

    def e_more(_):
        arrived(e_z)
        mine = eg.at[my_rows[0]]
        for off in (2, 1, 3):
            put(e_y, mine, mine, {"y": at_off("y", off)})

    def e_fin(_):
        arrived(e_y)
        e_t = jnp.transpose(eg[...].reshape(T, EXT).astype(F32)).astype(BF16)
        for k in range(2):
            o_gl[k] = SCALE * nn(e_t[64 * k:64 * k + 64], xc[0].reshape(T, DS))
        o_do[...] = SCALE * nn(e_t[128:192], xc[1].reshape(T, DS))
        e2 = 2.0 * eg[me["x"], pl.ds(2 * me["c"], 2)].reshape(32, EXT)
        lora[0] = nn(e2[:, 128:256], cw[...])
        lora[1] = nn(e2[:, 0:128], aw[...])

    pair = [group(qt.at[n]) for n in range(2)]
    b_x = [group(rx.at[n]) for n in range(2)]
    accs, res = (acc_o, acc_i), (o_out, o_in)

    def rows_of(xi, c):
        return pl.ds(pl.multiple_of((xi * 2 + c) * 32, 32), 32)

    def pair_send(n):
        for xi in range(X):
            qt[n, xi] = accs[n][rows_of(xi, other), :].astype(BF16)
        put(pair[n], qt.at[n], rt.at[n], {"c": other})

    def x_send(n):
        arrived(pair[n])
        for off in (2, 1, 3):
            xi = at_off("x", off)
            v = accs[n][rows_of(xi, me["c"]), :] + rt[n, xi].astype(F32)
            uq[n, off - 1] = v.astype(BF16)
            put(b_x[n], uq.at[n, off - 1], rx.at[n, off - 1], {"x": xi})

    def x_fin(n):
        v = accs[n][rows_of(me["x"], me["c"]), :] + rt[n, me["x"]].astype(F32) + lora[n]
        arrived(b_x[n])
        for k in range(3):
            v = v + rx[n, k].astype(F32)
        res[n][...] = v.astype(BF16)

    steps = {"gu": compute_gu, "hb": compute_hb, "send": rs1_send, "agg": rs1_agg, "sum": rs1_fin,
             "mid": middle, "spread": ag2_send, "fwd": ag2_fwd, "fin": ag2_fin,
             "out": post_o, "in": post_i, "flip": flip, "grad": grads,
             "esend": e_send, "esum": e_sum, "emore": e_more, "efin": e_fin,
             "pair": pair_send, "xsend": x_send, "xfin": x_fin}
    for step, s in SCHEDULE:
        with jax.named_scope(step + str(s)):
            steps[step](s)
    for n in range(len(departures)):
        sent(n)
    assert (len(arrivals), len(departures)) == (N_RECV, N_SENT), (len(arrivals), len(departures))


RESULTS = (
    ((32, DS), BF16), ((32, DS), BF16), ((2, R, DS), F32),
    ((2, R, FS), F32), ((R, FS), F32), ((R, DS), F32),
)


def store(*refs):
    copies = [pltpu.make_async_copy(refs[n], refs[6 + n], refs[12].at[n]) for n in (3, 4, 2, 5, 0, 1)]
    for c in copies:
        c.start()
    for c in copies:
        c.wait()


def per_device(tok, w, wd, a, b, din, dout, cot):
    at = jnp.swapaxes(a, 1, 2).reshape(2 * R, DS)
    dint = jnp.swapaxes(din, 0, 1)
    vm = pltpu.VMEM
    scratch = [
        vm((2, X * C, 32, DS), BF16), vm((2, DS, FS), BF16), vm((FS, DS), BF16),
        vm((128, DS), BF16), vm((128, DS), BF16), vm((3, 128, FS), BF16),
        vm((T, DS), F32), vm((T, DS), F32),
        vm((16, EXT), BF16), vm((16, EXT), F32), vm((EXT, T), BF16), vm((2, 32, DS), F32),
        vm((2, X, 32, DS), BF16), vm((2, X, 32, DS), BF16),
        vm((2, 3, 32, DS), BF16), vm((2, 3, 32, DS), BF16),
        vm((16, EXT), BF16), vm((7, 16, EXT), BF16), vm((4, 3, 16, EXT), BF16), vm((Y, Z, 16, EXT), BF16),
        vm((4, 32, DS), BF16), vm((30, 16, max(WIDTHS)), BF16),
    ]
    for wid in WIDTHS:
        scratch += [
            vm((Y, Z, 16, wid), F32), vm((Y, Z, 16, wid), BF16),
            vm((2, 2, 16, wid), BF16), vm((2, 2, 16, wid), BF16), vm((2, 4, 16, wid), BF16),
            vm((4, 16, wid), F32), vm((4, 16, wid), BF16), vm((3, 16, wid), BF16),
            vm((Y, Z, 16, wid), BF16),
        ]
    scratch += [pltpu.SemaphoreType.DMA((9,)), pltpu.SemaphoreType.DMA((N_SENT,)), pltpu.SemaphoreType.DMA((N_RECV,))]
    anyspec = pl.BlockSpec(memory_space=pltpu.MemorySpace.HBM)
    vspec = pl.BlockSpec(memory_space=pltpu.VMEM)
    res = pl.pallas_call(
        body,
        out_shape=tuple(vm(s, d) for s, d in RESULTS),
        in_specs=[anyspec] * 8,
        out_specs=(vspec,) * 6,
        scratch_shapes=scratch,
        compiler_params=pltpu.CompilerParams(
            collective_id=0, has_side_effects=True, vmem_limit_bytes=40 * 1024 * 1024),
        name="layer",
    )(*(pltpu.with_memory_space_constraint(v, pltpu.MemorySpace.HBM)
        for v in (tok, w, wd, at, b, dint, dout, cot)))
    out, inp, gl, gf, di, do = pl.pallas_call(
        store,
        out_shape=tuple(jax.ShapeDtypeStruct(s, d) for s, d in RESULTS),
        in_specs=[vspec] * 6,
        out_specs=(anyspec,) * 6,
        scratch_shapes=[pltpu.SemaphoreType.DMA((6,))],
        compiler_params=pltpu.CompilerParams(vmem_limit_bytes=1024 * 1024),
        name="store",
    )(*res)
    return out, inp, jnp.swapaxes(gl, 1, 2), gf, jnp.swapaxes(di, 0, 1), do


def solution(mesh):
    torus = Mesh(mesh.devices.reshape(X, C, Y, Z), ("x", "c", "y", "z"))
    dp, mp = ("x", "c"), ("y", "z")
    in_specs = (
        P(dp, mp), P(None, mp, dp), P(dp, mp), P(None, mp, None),
        P(None, None, dp), P(dp, None), P(None, mp), P(dp, mp),
    )
    out_specs = (P(dp, mp), P(dp, mp), P(None, mp, None), P(None, None, dp), P(dp, None), P(None, mp))
    return jax.shard_map(per_device, mesh=torus, in_specs=in_specs, out_specs=out_specs, check_vma=False)
```

```python
import math

import jax
import jax.numpy as jnp
from jax import lax
from jax.experimental import pallas as pl
from jax.experimental.pallas import tpu as pltpu
from jax.sharding import Mesh
from jax.sharding import PartitionSpec as P

MESH = pl.DeviceIdType.MESH
F32 = jnp.float32
BF16 = jnp.bfloat16

X, C, Y, Z = 4, 2, 4, 4
T = 256
DS = 512
FS = 1920
R = 64
EXT = 256
SCALE = 2.0 * T ** -0.5

SUBS = (
    ("z", 1024, 128, True), ("y", 0, 256, False), ("z", 1152, 256, False), ("y", 256, 256, False),
    ("z", 1408, 256, False), ("y", 512, 256, False), ("z", 1664, 256, False), ("y", 768, 256, False),
)
WIDTHS = tuple(3 * hw + (EXT if ext else 0) for _, _, hw, ext in SUBS)
HALVES = {"y": (0, 1024, 1024), "z": (1024, 896, 896 + EXT)}
NS = len(SUBS)
N_RECV = 17 + 6 * NS
TILE = 16 * 128
SENT_TILES = 30 * sum(WIDTHS) // 128 + 268
LOAD_TILES = (3 * R * DS + 3 * R * FS + 3 * DS * FS) // TILE


def steps_of(subs, *names):
    return [(name, s) for s in subs for name in names]


SCHEDULE = (
    steps_of(range(3), "gu", "sendgu") + steps_of(range(3), "hb", "sendhb")
    + steps_of(range(3, NS), "gu", "sendgu", "hb", "sendhb")
    + steps_of(range(NS), "agg") + steps_of(range(NS), "sum") + steps_of(range(NS), "mid", "near")
    + [("esend", 0)] + steps_of(range(4), "spread") + steps_of(range(2), "hspread") + steps_of(range(4, 6), "spread")
    + steps_of(range(2), "hfwd") + steps_of(range(6, NS), "spread") + steps_of(range(4), "fwd")
    + [("esum", 0)] + steps_of(range(4, 6), "fwd")
    + [("hfin", 0), ("hfin", 1), ("out", 0), ("pair", 0)]
    + steps_of(range(6, NS), "fwd") + steps_of(range(2), "fin", "in") + [("xsend", 0)]
    + steps_of(range(2, 4), "fin", "in") + [("emore", 0)]
    + steps_of(range(4, NS), "fin", "in") + [("pair", 1), ("flip", 0), ("hgrad", 0)]
    + steps_of(range(3), "grad") + [("xsend", 1)] + steps_of(range(3, NS), "grad")
    + [("efin", 0), ("xfin", 0), ("xfin", 1)]
)


def nn(a, b):
    return jnp.dot(a, b, preferred_element_type=F32)


def nt(a, b):
    return lax.dot_general(a, b, (((1,), (1,)), ((), ())), preferred_element_type=F32)


def body(tok, w_hbm, wd_hbm, at_hbm, b_hbm, dint_hbm, dout_hbm, cot,
         o_out, o_in, o_gl, o_gf, o_di, o_do,
         xc, w, wd, aw, cw, ew, acc_o, acc_i, ext2, e_acc, ext_t, lora,
         qt, rt, uq, rx, e_out, e_in, eg, bytes_ref, h_y, h_z, *rest):
    per = len(rest) - 3
    each = per // NS
    bufs = [rest[s * each:(s + 1) * each] for s in range(NS)]
    local_sem, send_sem, recv_sem = rest[per:]
    me = {a: lax.axis_index(a) for a in ("x", "c", "y", "z")}

    def at_off(axis, off):
        return lax.rem(me[axis] + off, 4)

    arrivals, moved = [], [0]

    def bytes_of(tiles):
        return bytes_ref.at[0:tiles]

    def group(like):
        arrivals.append(like)
        return len(arrivals) - 1

    def put(g, src, dst, device):
        moved[0] += math.prod(src.shape) // TILE
        pltpu.make_async_remote_copy(
            src_ref=src, dst_ref=dst, send_sem=send_sem, recv_sem=recv_sem.at[g],
            device_id=device, device_id_type=MESH).start()

    def arrived(g):
        size = bytes_of(arrivals[g])
        pltpu.make_async_copy(size, size, recv_sem.at[g]).wait()

    other = 1 - me["c"]
    barrier = pltpu.get_barrier_semaphore()
    partners = [{"c": other}]
    for off in (1, 2, 3):
        partners += [{"x": at_off("x", off)}, {"x": at_off("x", off), "c": other},
                     {"y": at_off("y", off)}, {"z": at_off("z", off)}]
    for p in partners:
        pl.semaphore_signal(barrier, inc=1, device_id=p, device_id_type=MESH)

    my_dp = me["x"] * 2 + me["c"]
    loads = []
    for n, (src, dst) in enumerate(((tok, xc.at[0, my_dp]), (cot, xc.at[1, my_dp]))):
        loads.append(pltpu.make_async_copy(src, dst, local_sem.at[n]))
        loads[n].start()
    for src, dst in (
        (at_hbm, aw), (dout_hbm, cw.at[0:64]), (b_hbm.at[0], ew.at[0, 0:64]), (b_hbm.at[1], ew.at[1, 64:128]),
        (dint_hbm, ew.at[2, 0:64]), (w_hbm, w), (wd_hbm, wd),
    ):
        pltpu.make_async_copy(src, dst, local_sem.at[2]).start()
    cw[64:128, :] = jnp.zeros((64, DS), BF16)
    ew[0, 64:128, :] = jnp.zeros((64, FS), BF16)
    ew[1, 0:64, :] = jnp.zeros((64, FS), BF16)
    ew[2, 64:128, :] = jnp.zeros((64, FS), BF16)
    loads[0].wait()
    loads[1].wait()
    pl.semaphore_wait(barrier, len(partners))

    def block(n, off):
        return xc.at[n, at_off("x", off) * 2 + me["c"]]

    along = [group(3 * 8) for _ in range(2)]
    across = [group(4 * 8) for _ in range(2)]
    for n in range(2):
        for off in (2, 1, 3):
            put(along[n], block(n, 0), block(n, 0), {"x": at_off("x", off)})
        put(across[n], block(n, 0), block(n, 0), {"c": other})
    pltpu.make_async_copy(bytes_of(LOAD_TILES), bytes_of(LOAD_TILES), local_sem.at[2]).wait()
    for n in range(2):
        arrived(along[n])
        for off in (1, 2, 3):
            put(across[n], block(n, off), block(n, off), {"c": other})

    arrived(across[0])
    seen = set()

    def rows_all(n):
        return xc[n].reshape(T, DS)

    def seg(n, hw):
        return slice(n * hw, (n + 1) * hw)

    def keep(s, cols, v):
        v = v.reshape(Y, Z, 16, v.shape[-1])
        bufs[s][0][:, :, :, cols] = v
        bufs[s][1][:, :, :, cols] = v.astype(BF16)

    def compute_gu(s):
        _, f0, hw, _ = SUBS[s]
        cols = slice(f0, f0 + hw)
        for n in range(2):
            keep(s, seg(n, hw), nn(rows_all(0), w[n, :, cols]))

    def compute_hb(s):
        _, f0, hw, ext = SUBS[s]
        cols = slice(f0, f0 + hw)
        if "cot" not in seen:
            arrived(across[1])
            seen.add("cot")
        keep(s, seg(2, hw), nt(rows_all(1), wd[cols, :]))
        if ext:
            keep(s, slice(3 * hw, 3 * hw + 128), nt(rows_all(0), aw[...]))
            keep(s, slice(3 * hw + 128, 3 * hw + EXT), nt(rows_all(1), cw[...]))

    other_axis = {"y": "z", "z": "y"}

    def part(ref, a, a1, lo, hi, cols=slice(None)):
        if a == "y":
            return ref.at[a1, lo:hi, :, cols]
        return ref.at[lo:hi, a1, :, cols]

    def value(ref, s, a1, a2):
        if SUBS[s][0] == "y":
            return ref[a1, a2]
        return ref[a2, a1]

    st = []
    for s in range(NS):
        n, g = WIDTHS[s] // 128, 2 * SUBS[s][2] // 128
        st.append({"t": group(4 * n), "f": group(8 * n), "r": group(3 * n),
                   "a": group(3 * g), "t2": group(4 * g), "b": group(8 * g)})

    halves = {"y": h_y, "z": h_z}
    hst = {}
    for a, (_, _, n) in HALVES.items():
        hst[a] = {"a": group(3 * n // 128), "t2": group(4 * n // 128), "b": group(8 * n // 128)}

    def ring(s):
        a = SUBS[s][0]
        return a, {a: at_off(a, 3)}, {a: at_off(a, 1)}

    def rs1_send(s, cols):
        a, left, right = ring(s)
        q, tt, ff = bufs[s][1], bufs[s][2], bufs[s][4]
        put(st[s]["t"], part(q, a, at_off(a, 2), 0, 2, cols), tt.at[0, :, :, cols], left)
        put(st[s]["t"], part(q, a, at_off(a, 2), 2, 4, cols), tt.at[1, :, :, cols], right)
        put(st[s]["f"], part(q, a, at_off(a, 3), 2, 4, cols), ff.at[0, 2:4, :, cols], left)
        put(st[s]["f"], part(q, a, at_off(a, 1), 0, 2, cols), ff.at[1, 0:2, :, cols], right)

    def rs1_agg(s):
        a, left, right = ring(s)
        p, tt, gg, ff = bufs[s][0], bufs[s][2], bufs[s][3], bufs[s][4]
        arrived(st[s]["t"])
        for j in range(2):
            gg[0, j] = (value(p, s, at_off(a, 3), j) + tt[0, j].astype(F32)).astype(BF16)
        put(st[s]["f"], gg.at[0], ff.at[0, 0:2], left)
        for j in range(2):
            gg[1, j] = (value(p, s, at_off(a, 1), 2 + j) + tt[1, j].astype(F32)).astype(BF16)
        put(st[s]["f"], gg.at[1], ff.at[1, 2:4], right)

    def rs1_fin(s):
        a = SUBS[s][0]
        b = other_axis[a]
        p, ff, sm, q2, r2 = (bufs[s][k] for k in (0, 4, 5, 6, 7))
        arrived(st[s]["f"])
        for j in range(4):
            v = value(p, s, me[a], j) + ff[0, j].astype(F32) + ff[1, j].astype(F32)
            sm[j] = v
            q2[j] = v.astype(BF16)
        for off in (2, 1, 3):
            put(st[s]["r"], q2.at[at_off(b, off)], r2.at[off - 1], {b: at_off(b, off)})

    def add(ref, key, v):
        if key in seen:
            v = v + ref[...]
        seen.add(key)
        ref[...] = v

    def middle(s):
        a, f0, hw, ext = SUBS[s]
        b = other_axis[a]
        sm, r2, act = (bufs[s][k] for k in (5, 7, 8))
        hid_ref, h0 = halves[a], f0 - HALVES[a][0]
        arrived(st[s]["r"])

        def total(cols):
            v = sm[me[b], :, cols]
            for n in range(3):
                v = v + r2[n, :, cols].astype(F32)
            return v

        my = (me["y"], me["z"])
        cols = slice(f0, f0 + hw)
        if ext:
            v = total(slice(3 * hw, 3 * hw + EXT)).astype(BF16)
            hid_ref[my[0], my[1], :, HALVES[a][1]:] = v
            ext2[...] = 2.0 * v
        lows = (ext2[:, 0:128], ext2[:, 0:128], ext2[:, 128:256])
        gate, up, hb = (total(seg(n, hw)) + nn(lows[n], ew[n, :, cols]) for n in range(3))
        sg = 1.0 / (1.0 + jnp.exp(-gate))
        gs = gate * sg
        hid = (gs * up).astype(BF16)
        gb = (hb * up * sg * (1.0 + gate * (1.0 - sg))).astype(BF16)
        ub = (hb * gs).astype(BF16)
        hid_ref[my[0], my[1], :, h0:h0 + hw] = hid
        act[my[0], my[1], :, seg(0, hw)] = gb
        act[my[0], my[1], :, seg(1, hw)] = ub
        pieces = [slice(h0, h0 + hw)] + ([slice(HALVES[a][1], HALVES[a][1] + EXT)] if ext else [])
        for piece in pieces:
            mine = hid_ref.at[my[0], my[1], :, piece]
            for off in (2, 1, 3):
                put(hst[a]["a"], mine, mine, {b: at_off(b, off)})
        add(e_acc.at[:, 0:128], "bl", nt(gb, ew[0, :, cols]) + nt(ub, ew[1, :, cols]))
        add(e_acc.at[:, 128:256], "ld", nt(hid, ew[2, :, cols]))

    def near(s):
        b = other_axis[SUBS[s][0]]
        mine = bufs[s][8].at[me["y"], me["z"]]
        for off in (2, 1, 3):
            put(st[s]["a"], mine, mine, {b: at_off(b, off)})

    def spread(ref, a, groups):
        left, right = {a: at_off(a, 3)}, {a: at_off(a, 1)}
        arrived(groups["a"])
        lo, hi = part(ref, a, me[a], 0, 2), part(ref, a, me[a], 2, 4)
        put(groups["t2"], lo, lo, left)
        put(groups["t2"], hi, hi, right)
        put(groups["b"], hi, hi, left)
        put(groups["b"], lo, lo, right)

    def forward(ref, a, groups):
        left, right = {a: at_off(a, 3)}, {a: at_off(a, 1)}
        arrived(groups["t2"])
        src = part(ref, a, at_off(a, 1), 0, 2)
        put(groups["b"], src, src, left)
        src = part(ref, a, at_off(a, 3), 2, 4)
        put(groups["b"], src, src, right)

    def all_rows(ref, cols):
        return ref[:, :, :, cols].reshape(T, cols.stop - cols.start)

    def post_o(_):
        v = [nn(all_rows(halves[a], slice(0, n)), wd[f0:f0 + n, :]) for a, (f0, n, _) in HALVES.items()]
        acc_o[...] = v[0] + v[1]

    def post_i(s):
        _, f0, hw, _ = SUBS[s]
        cols = slice(f0, f0 + hw)
        act = bufs[s][8]
        add(acc_i, "i", nt(all_rows(act, seg(0, hw)), w[0, :, cols]) + nt(all_rows(act, seg(1, hw)), w[1, :, cols]))

    def flip(_):
        n = HALVES["z"][1]
        ext_t[...] = jnp.transpose(all_rows(h_z, slice(n, n + EXT)).astype(F32)).astype(BF16)

    def h_grads(_):
        for a, (f0, n, _) in HALVES.items():
            o_di[:, f0:f0 + n] = SCALE * nn(ext_t[128:192, :], all_rows(halves[a], slice(0, n)))

    def grads(s):
        _, f0, hw, _ = SUBS[s]
        cols = slice(f0, f0 + hw)
        for k in range(2):
            o_gf[k, :, cols] = SCALE * nn(ext_t[64 * k:64 * k + 64, :], all_rows(bufs[s][8], seg(k, hw)))

    my_rows = (me["y"], me["z"])
    e_dp, e_z, e_y = group(7 * 2), group(3 * 2), group(12 * 2)
    hops = [(off, d) for off in (2, 1, 3, 0) for d in (0, 1) if off or d]

    def e_send(_):
        e_out[...] = e_acc[...].astype(BF16)
        for n, (off, d) in enumerate(hops):
            put(e_dp, e_out, e_in.at[n], {"x": at_off("x", off), "c": lax.rem(me["c"] + d, 2)})

    def e_sum(_):
        arrived(e_dp)
        v = e_acc[...]
        for n in range(7):
            v = v + e_in[n].astype(F32)
        eg[my_rows[0], my_rows[1]] = v.astype(BF16)
        mine = eg.at[my_rows[0], my_rows[1]]
        for off in (2, 1, 3):
            put(e_z, mine, mine, {"z": at_off("z", off)})

    def e_more(_):
        arrived(e_z)
        mine = eg.at[my_rows[0]]
        for off in (2, 1, 3):
            put(e_y, mine, mine, {"y": at_off("y", off)})

    def e_fin(_):
        arrived(e_y)
        e_t = jnp.transpose(eg[...].reshape(T, EXT).astype(F32)).astype(BF16)
        for k in range(2):
            o_gl[k] = SCALE * nn(e_t[64 * k:64 * k + 64], xc[0].reshape(T, DS))
        o_do[...] = SCALE * nn(e_t[128:192], xc[1].reshape(T, DS))
        e2 = 2.0 * eg[me["x"], pl.ds(2 * me["c"], 2)].reshape(32, EXT)
        lora[0] = nn(e2[:, 128:256], cw[...])
        lora[1] = nn(e2[:, 0:128], aw[...])

    pair = [group(4 * 8) for n in range(2)]
    b_x = [group(3 * 8) for n in range(2)]
    accs, res = (acc_o, acc_i), (o_out, o_in)

    def rows_of(xi, c):
        return pl.ds(pl.multiple_of((xi * 2 + c) * 32, 32), 32)

    def pair_send(n):
        for xi in range(X):
            qt[n, xi] = accs[n][rows_of(xi, other), :].astype(BF16)
        put(pair[n], qt.at[n], rt.at[n], {"c": other})

    def x_send(n):
        arrived(pair[n])
        for off in (2, 1, 3):
            xi = at_off("x", off)
            v = accs[n][rows_of(xi, me["c"]), :] + rt[n, xi].astype(F32)
            uq[n, off - 1] = v.astype(BF16)
            put(b_x[n], uq.at[n, off - 1], rx.at[n, off - 1], {"x": xi})

    def x_fin(n):
        v = accs[n][rows_of(me["x"], me["c"]), :] + rt[n, me["x"]].astype(F32) + lora[n]
        arrived(b_x[n])
        for k in range(3):
            v = v + rx[n, k].astype(F32)
        res[n][...] = v.astype(BF16)

    def on_sub(fn):
        return lambda s: fn(bufs[s][8], SUBS[s][0], st[s])

    def on_half(fn):
        return lambda n: fn(halves["zy"[n]], "zy"[n], hst["zy"[n]])

    steps = {"gu": compute_gu, "hb": compute_hb, "sendgu": lambda s: rs1_send(s, slice(0, 2 * SUBS[s][2])),
             "sendhb": lambda s: rs1_send(s, slice(2 * SUBS[s][2], WIDTHS[s])), "agg": rs1_agg, "sum": rs1_fin,
             "mid": middle, "near": near, "spread": on_sub(spread), "fwd": on_sub(forward),
             "fin": lambda s: arrived(st[s]["b"]), "hspread": on_half(spread), "hfwd": on_half(forward),
             "hfin": lambda n: arrived(hst["zy"[n]]["b"]),
             "out": post_o, "in": post_i, "flip": flip, "grad": grads, "hgrad": h_grads,
             "esend": e_send, "esum": e_sum, "emore": e_more, "efin": e_fin,
             "pair": pair_send, "xsend": x_send, "xfin": x_fin}
    for step, s in SCHEDULE:
        with jax.named_scope(step + str(s)):
            steps[step](s)
    pltpu.make_async_copy(bytes_of(SENT_TILES), bytes_of(SENT_TILES), send_sem).wait()
    assert (len(arrivals), moved[0]) == (N_RECV, SENT_TILES), (len(arrivals), moved[0])


RESULTS = (
    ((32, DS), BF16), ((32, DS), BF16), ((2, R, DS), F32),
    ((2, R, FS), F32), ((R, FS), F32), ((R, DS), F32),
)


def store(*refs):
    copies = [pltpu.make_async_copy(refs[n], refs[6 + n], refs[12].at[n]) for n in (3, 4, 2, 5, 0, 1)]
    for c in copies:
        c.start()
    for c in copies:
        c.wait()


def per_device(tok, w, wd, a, b, din, dout, cot):
    at = jnp.swapaxes(a, 1, 2).reshape(2 * R, DS)
    dint = jnp.swapaxes(din, 0, 1)
    vm = pltpu.VMEM
    scratch = [
        vm((2, X * C, 32, DS), BF16), vm((2, DS, FS), BF16), vm((FS, DS), BF16),
        vm((128, DS), BF16), vm((128, DS), BF16), vm((3, 128, FS), BF16),
        vm((T, DS), F32), vm((T, DS), F32),
        vm((16, EXT), BF16), vm((16, EXT), F32), vm((EXT, T), BF16), vm((2, 32, DS), F32),
        vm((2, X, 32, DS), BF16), vm((2, X, 32, DS), BF16),
        vm((2, 3, 32, DS), BF16), vm((2, 3, 32, DS), BF16),
        vm((16, EXT), BF16), vm((7, 16, EXT), BF16), vm((Y, Z, 16, EXT), BF16),
        vm((max(SENT_TILES, LOAD_TILES), 16, 128), BF16),
        vm((Y, Z, 16, HALVES["y"][2]), BF16), vm((Y, Z, 16, HALVES["z"][2]), BF16),
    ]
    for wid, (_, _, hw, _) in zip(WIDTHS, SUBS):
        scratch += [
            vm((Y, Z, 16, wid), F32), vm((Y, Z, 16, wid), BF16),
            vm((2, 2, 16, wid), BF16), vm((2, 2, 16, wid), BF16), vm((2, 4, 16, wid), BF16),
            vm((4, 16, wid), F32), vm((4, 16, wid), BF16), vm((3, 16, wid), BF16),
            vm((Y, Z, 16, 2 * hw), BF16),
        ]
    scratch += [pltpu.SemaphoreType.DMA((3,)), pltpu.SemaphoreType.DMA, pltpu.SemaphoreType.DMA((N_RECV,))]
    anyspec = pl.BlockSpec(memory_space=pltpu.MemorySpace.HBM)
    vspec = pl.BlockSpec(memory_space=pltpu.VMEM)
    res = pl.pallas_call(
        body,
        out_shape=tuple(vm(s, d) for s, d in RESULTS),
        in_specs=[anyspec] * 8,
        out_specs=(vspec,) * 6,
        scratch_shapes=scratch,
        compiler_params=pltpu.CompilerParams(
            collective_id=0, has_side_effects=True, vmem_limit_bytes=40 * 1024 * 1024),
        name="layer",
    )(*(pltpu.with_memory_space_constraint(v, pltpu.MemorySpace.HBM)
        for v in (tok, w, wd, at, b, dint, dout, cot)))
    out, inp, gl, gf, di, do = pl.pallas_call(
        store,
        out_shape=tuple(jax.ShapeDtypeStruct(s, d) for s, d in RESULTS),
        in_specs=[vspec] * 6,
        out_specs=(anyspec,) * 6,
        scratch_shapes=[pltpu.SemaphoreType.DMA((6,))],
        compiler_params=pltpu.CompilerParams(vmem_limit_bytes=1024 * 1024),
        name="store",
    )(*res)
    return out, inp, jnp.swapaxes(gl, 1, 2), gf, jnp.swapaxes(di, 0, 1), do


def solution(mesh):
    torus = Mesh(mesh.devices.reshape(X, C, Y, Z), ("x", "c", "y", "z"))
    dp, mp = ("x", "c"), ("y", "z")
    in_specs = (
        P(dp, mp), P(None, mp, dp), P(dp, mp), P(None, mp, None),
        P(None, None, dp), P(dp, None), P(None, mp), P(dp, mp),
    )
    out_specs = (P(dp, mp), P(dp, mp), P(None, mp, None), P(None, None, dp), P(dp, None), P(None, mp))
    return jax.shard_map(per_device, mesh=torus, in_specs=in_specs, out_specs=out_specs, check_vma=False)
```

```python
import math

import jax
import jax.numpy as jnp
from jax import lax
from jax.experimental import pallas as pl
from jax.experimental.pallas import tpu as pltpu
from jax.sharding import Mesh
from jax.sharding import PartitionSpec as P

MESH = pl.DeviceIdType.MESH
F32 = jnp.float32
BF16 = jnp.bfloat16

X, C, Y, Z = 4, 2, 4, 4
T = 256
DS = 512
FS = 1920
R = 64
EXT = 256
SCALE = 2.0 * T ** -0.5

SUBS = (
    ("z", 1024, 128, True), ("y", 0, 256, False), ("z", 1152, 256, False), ("y", 256, 256, False),
    ("z", 1408, 256, False), ("y", 512, 256, False), ("z", 1664, 256, False), ("y", 768, 256, False),
)
WIDTHS = tuple(3 * hw + (EXT if ext else 0) for _, _, hw, ext in SUBS)
HALVES = {"y": (0, 1024, 1024), "z": (1024, 896, 896 + EXT)}
NS = len(SUBS)
N_RECV = 17 + 4 * NS
TILE = 16 * 128
SENT_TILES = 30 * sum(WIDTHS) // 128 + 268
LOAD_TILES = (3 * R * DS + 3 * R * FS + 3 * DS * FS) // TILE


def steps_of(subs, *names):
    return [(name, s) for s in subs for name in names]


SCHEDULE = (
    steps_of(range(3), "gu", "sendgu") + steps_of(range(3), "hb", "sendhb")
    + steps_of(range(3, NS), "gu", "sendgu", "hb", "sendhb")
    + steps_of(range(NS), "agg") + steps_of(range(NS), "sum") + steps_of(range(NS), "mid")
    + [("esend", 0)] + steps_of(range(4), "spread") + steps_of(range(2), "hspread") + steps_of(range(4, 6), "spread")
    + steps_of(range(2), "hfwd") + steps_of(range(6, NS), "spread") + steps_of(range(4), "fwd")
    + [("esum", 0)] + steps_of(range(4, 6), "fwd")
    + [("hfin", 0), ("hfin", 1)] + steps_of(range(6, NS), "fwd") + [("out", 0), ("pair", 0)]
    + steps_of(range(2), "fin", "in") + [("xsend", 0)]
    + steps_of(range(2, 4), "fin", "in") + [("emore", 0)]
    + steps_of(range(4, NS), "fin", "in") + [("pair", 1), ("flip", 0), ("hgrad", 0)]
    + steps_of(range(3), "grad") + [("xsend", 1)] + steps_of(range(3, NS), "grad")
    + [("efin", 0), ("xfin", 0), ("xfin", 1)]
)


def nn(a, b):
    return jnp.dot(a, b, preferred_element_type=F32)


def nt(a, b):
    return lax.dot_general(a, b, (((1,), (1,)), ((), ())), preferred_element_type=F32)


def body(tok, w_hbm, wd_hbm, at_hbm, b_hbm, dint_hbm, dout_hbm, cot,
         o_out, o_in, o_gl, o_gf, o_di, o_do,
         xc, w, wd, aw, cw, ew, acc_o, acc_i, ext2, e_acc, ext_t, lora,
         qt, rt, uq, rx, e_out, e_in, eg, bytes_ref, h_y, h_z, *rest):
    per = len(rest) - 3
    each = per // NS
    bufs = [rest[s * each:(s + 1) * each] for s in range(NS)]
    local_sem, send_sem, recv_sem = rest[per:]
    me = {a: lax.axis_index(a) for a in ("x", "c", "y", "z")}

    def at_off(axis, off):
        return lax.rem(me[axis] + off, 4)

    arrivals, moved = [], [0]

    def bytes_of(tiles):
        return bytes_ref.at[0:tiles]

    def group(like, same=None):
        if same is not None:
            return same[0], like
        arrivals.append(like)
        return len(arrivals) - 1, like

    def put(g, src, dst, device):
        moved[0] += math.prod(src.shape) // TILE
        pltpu.make_async_remote_copy(
            src_ref=src, dst_ref=dst, send_sem=send_sem, recv_sem=recv_sem.at[g[0]],
            device_id=device, device_id_type=MESH).start()

    def arrived(g):
        size = bytes_of(g[1])
        pltpu.make_async_copy(size, size, recv_sem.at[g[0]]).wait()

    other = 1 - me["c"]
    barrier = pltpu.get_barrier_semaphore()
    partners = [{"c": other}]
    for off in (1, 2, 3):
        partners += [{"x": at_off("x", off)}, {"x": at_off("x", off), "c": other},
                     {"y": at_off("y", off)}, {"z": at_off("z", off)}]
    for p in partners:
        pl.semaphore_signal(barrier, inc=1, device_id=p, device_id_type=MESH)

    my_dp = me["x"] * 2 + me["c"]
    loads = []
    for n, (src, dst) in enumerate(((tok, xc.at[0, my_dp]), (cot, xc.at[1, my_dp]))):
        loads.append(pltpu.make_async_copy(src, dst, local_sem.at[n]))
        loads[n].start()
    for src, dst in (
        (at_hbm, aw), (dout_hbm, cw.at[0:64]), (b_hbm.at[0], ew.at[0, 0:64]), (b_hbm.at[1], ew.at[1, 64:128]),
        (dint_hbm, ew.at[2, 0:64]), (w_hbm, w), (wd_hbm, wd),
    ):
        pltpu.make_async_copy(src, dst, local_sem.at[2]).start()
    cw[64:128, :] = jnp.zeros((64, DS), BF16)
    ew[0, 64:128, :] = jnp.zeros((64, FS), BF16)
    ew[1, 0:64, :] = jnp.zeros((64, FS), BF16)
    ew[2, 64:128, :] = jnp.zeros((64, FS), BF16)
    loads[0].wait()
    loads[1].wait()
    pl.semaphore_wait(barrier, len(partners))

    def block(n, off):
        return xc.at[n, at_off("x", off) * 2 + me["c"]]

    along = [group(3 * 8) for _ in range(2)]
    across = [group(4 * 8) for _ in range(2)]
    for n in range(2):
        for off in (2, 1, 3):
            put(along[n], block(n, 0), block(n, 0), {"x": at_off("x", off)})
        put(across[n], block(n, 0), block(n, 0), {"c": other})
    pltpu.make_async_copy(bytes_of(LOAD_TILES), bytes_of(LOAD_TILES), local_sem.at[2]).wait()
    for n in range(2):
        arrived(along[n])
        for off in (1, 2, 3):
            put(across[n], block(n, off), block(n, off), {"c": other})

    arrived(across[0])
    seen = set()

    def rows_all(n):
        return xc[n].reshape(T, DS)

    def seg(n, hw):
        return slice(n * hw, (n + 1) * hw)

    def keep(s, cols, v):
        v = v.reshape(Y, Z, 16, v.shape[-1])
        bufs[s][0][:, :, :, cols] = v
        bufs[s][1][:, :, :, cols] = v.astype(BF16)

    def compute_gu(s):
        _, f0, hw, _ = SUBS[s]
        cols = slice(f0, f0 + hw)
        for n in range(2):
            keep(s, seg(n, hw), nn(rows_all(0), w[n, :, cols]))

    def compute_hb(s):
        _, f0, hw, ext = SUBS[s]
        cols = slice(f0, f0 + hw)
        if "cot" not in seen:
            arrived(across[1])
            seen.add("cot")
        keep(s, seg(2, hw), nt(rows_all(1), wd[cols, :]))
        if ext:
            keep(s, slice(3 * hw, 3 * hw + 128), nt(rows_all(0), aw[...]))
            keep(s, slice(3 * hw + 128, 3 * hw + EXT), nt(rows_all(1), cw[...]))

    other_axis = {"y": "z", "z": "y"}

    def part(ref, a, a1, lo, hi, cols=slice(None)):
        if a == "y":
            return ref.at[a1, lo:hi, :, cols]
        return ref.at[lo:hi, a1, :, cols]

    def value(ref, s, a1, a2):
        if SUBS[s][0] == "y":
            return ref[a1, a2]
        return ref[a2, a1]

    st = []
    for s in range(NS):
        n, g = WIDTHS[s] // 128, 2 * SUBS[s][2] // 128
        t, f = group(4 * n), group(8 * n)
        st.append({"t": t, "f": f, "r": group(3 * n), "a": group(3 * g, f),
                   "t2": group(4 * g, t), "b": group(8 * g)})

    halves = {"y": h_y, "z": h_z}
    hst = {}
    for a, (_, _, n) in HALVES.items():
        hst[a] = {"a": group(3 * n // 128), "t2": group(4 * n // 128), "b": group(8 * n // 128)}

    def ring(s):
        a = SUBS[s][0]
        return a, {a: at_off(a, 3)}, {a: at_off(a, 1)}

    def rs1_send(s, cols):
        a, left, right = ring(s)
        q, tt, ff = bufs[s][1], bufs[s][2], bufs[s][4]
        put(st[s]["t"], part(q, a, at_off(a, 2), 0, 2, cols), tt.at[0, :, :, cols], left)
        put(st[s]["t"], part(q, a, at_off(a, 2), 2, 4, cols), tt.at[1, :, :, cols], right)
        put(st[s]["f"], part(q, a, at_off(a, 3), 2, 4, cols), ff.at[0, 2:4, :, cols], left)
        put(st[s]["f"], part(q, a, at_off(a, 1), 0, 2, cols), ff.at[1, 0:2, :, cols], right)

    def rs1_agg(s):
        a, left, right = ring(s)
        p, tt, gg, ff = bufs[s][0], bufs[s][2], bufs[s][3], bufs[s][4]
        arrived(st[s]["t"])
        for j in range(2):
            gg[0, j] = (value(p, s, at_off(a, 3), j) + tt[0, j].astype(F32)).astype(BF16)
        put(st[s]["f"], gg.at[0], ff.at[0, 0:2], left)
        for j in range(2):
            gg[1, j] = (value(p, s, at_off(a, 1), 2 + j) + tt[1, j].astype(F32)).astype(BF16)
        put(st[s]["f"], gg.at[1], ff.at[1, 2:4], right)

    def rs1_fin(s):
        a = SUBS[s][0]
        b = other_axis[a]
        p, ff, sm, q2, r2 = (bufs[s][k] for k in (0, 4, 5, 6, 7))
        arrived(st[s]["f"])
        for j in range(4):
            v = value(p, s, me[a], j) + ff[0, j].astype(F32) + ff[1, j].astype(F32)
            sm[j] = v
            q2[j] = v.astype(BF16)
        for off in (2, 1, 3):
            put(st[s]["r"], q2.at[at_off(b, off)], r2.at[off - 1], {b: at_off(b, off)})

    def add(ref, key, v):
        if key in seen:
            v = v + ref[...]
        seen.add(key)
        ref[...] = v

    def middle(s):
        a, f0, hw, ext = SUBS[s]
        b = other_axis[a]
        sm, r2, act = (bufs[s][k] for k in (5, 7, 8))
        hid_ref, h0 = halves[a], f0 - HALVES[a][0]
        arrived(st[s]["r"])

        def total(cols):
            v = sm[me[b], :, cols]
            for n in range(3):
                v = v + r2[n, :, cols].astype(F32)
            return v

        my = (me["y"], me["z"])
        cols = slice(f0, f0 + hw)
        if ext:
            v = total(slice(3 * hw, 3 * hw + EXT)).astype(BF16)
            hid_ref[my[0], my[1], :, HALVES[a][1]:] = v
            ext2[...] = 2.0 * v
        lows = (ext2[:, 0:128], ext2[:, 0:128], ext2[:, 128:256])
        gate, up, hb = (total(seg(n, hw)) + nn(lows[n], ew[n, :, cols]) for n in range(3))
        sg = 1.0 / (1.0 + jnp.exp(-gate))
        gs = gate * sg
        hid = (gs * up).astype(BF16)
        gb = (hb * up * sg * (1.0 + gate * (1.0 - sg))).astype(BF16)
        ub = (hb * gs).astype(BF16)
        hid_ref[my[0], my[1], :, h0:h0 + hw] = hid
        act[my[0], my[1], :, seg(0, hw)] = gb
        act[my[0], my[1], :, seg(1, hw)] = ub
        pieces = [slice(h0, h0 + hw)] + ([slice(HALVES[a][1], HALVES[a][1] + EXT)] if ext else [])
        for piece in pieces:
            mine = hid_ref.at[my[0], my[1], :, piece]
            for off in (2, 1, 3):
                put(hst[a]["a"], mine, mine, {b: at_off(b, off)})
        near(s)
        add(e_acc.at[:, 0:128], "bl", nt(gb, ew[0, :, cols]) + nt(ub, ew[1, :, cols]))
        add(e_acc.at[:, 128:256], "ld", nt(hid, ew[2, :, cols]))

    def near(s):
        b, mine = other_axis[SUBS[s][0]], bufs[s][8].at[me["y"], me["z"]]
        for off in (2, 1, 3):
            put(st[s]["a"], mine, mine, {b: at_off(b, off)})

    def spread(ref, a, groups):
        left, right = {a: at_off(a, 3)}, {a: at_off(a, 1)}
        arrived(groups["a"])
        lo, hi = part(ref, a, me[a], 0, 2), part(ref, a, me[a], 2, 4)
        put(groups["t2"], lo, lo, left)
        put(groups["t2"], hi, hi, right)
        put(groups["b"], hi, hi, left)
        put(groups["b"], lo, lo, right)

    def forward(ref, a, groups):
        left, right = {a: at_off(a, 3)}, {a: at_off(a, 1)}
        arrived(groups["t2"])
        src = part(ref, a, at_off(a, 1), 0, 2)
        put(groups["b"], src, src, left)
        src = part(ref, a, at_off(a, 3), 2, 4)
        put(groups["b"], src, src, right)

    def all_rows(ref, cols):
        return ref[:, :, :, cols].reshape(T, cols.stop - cols.start)

    def post_o(_):
        v = [nn(all_rows(halves[a], slice(0, n)), wd[f0:f0 + n, :]) for a, (f0, n, _) in HALVES.items()]
        acc_o[...] = v[0] + v[1]

    def post_i(s):
        _, f0, hw, _ = SUBS[s]
        cols = slice(f0, f0 + hw)
        act = bufs[s][8]
        add(acc_i, "i", nt(all_rows(act, seg(0, hw)), w[0, :, cols]) + nt(all_rows(act, seg(1, hw)), w[1, :, cols]))

    def flip(_):
        n = HALVES["z"][1]
        ext_t[...] = jnp.transpose(all_rows(h_z, slice(n, n + EXT)).astype(F32)).astype(BF16)

    def h_grads(_):
        for a, (f0, n, _) in HALVES.items():
            o_di[:, f0:f0 + n] = SCALE * nn(ext_t[128:192, :], all_rows(halves[a], slice(0, n)))

    def grads(s):
        _, f0, hw, _ = SUBS[s]
        cols = slice(f0, f0 + hw)
        for k in range(2):
            o_gf[k, :, cols] = SCALE * nn(ext_t[64 * k:64 * k + 64, :], all_rows(bufs[s][8], seg(k, hw)))

    my_rows = (me["y"], me["z"])
    e_dp, e_z, e_y = group(7 * 2), group(3 * 2), group(12 * 2)
    hops = [(off, d) for off in (2, 1, 3, 0) for d in (0, 1) if off or d]

    def e_send(_):
        e_out[...] = e_acc[...].astype(BF16)
        for n, (off, d) in enumerate(hops):
            put(e_dp, e_out, e_in.at[n], {"x": at_off("x", off), "c": lax.rem(me["c"] + d, 2)})

    def e_sum(_):
        arrived(e_dp)
        v = e_acc[...]
        for n in range(7):
            v = v + e_in[n].astype(F32)
        eg[my_rows[0], my_rows[1]] = v.astype(BF16)
        mine = eg.at[my_rows[0], my_rows[1]]
        for off in (2, 1, 3):
            put(e_z, mine, mine, {"z": at_off("z", off)})

    def e_more(_):
        arrived(e_z)
        mine = eg.at[my_rows[0]]
        for off in (2, 1, 3):
            put(e_y, mine, mine, {"y": at_off("y", off)})

    def e_fin(_):
        arrived(e_y)
        e_t = jnp.transpose(eg[...].reshape(T, EXT).astype(F32)).astype(BF16)
        for k in range(2):
            o_gl[k] = SCALE * nn(e_t[64 * k:64 * k + 64], xc[0].reshape(T, DS))
        o_do[...] = SCALE * nn(e_t[128:192], xc[1].reshape(T, DS))
        e2 = 2.0 * eg[me["x"], pl.ds(2 * me["c"], 2)].reshape(32, EXT)
        lora[0] = nn(e2[:, 128:256], cw[...])
        lora[1] = nn(e2[:, 0:128], aw[...])

    pair = [group(4 * 8) for n in range(2)]
    b_x = [group(3 * 8) for n in range(2)]
    accs, res = (acc_o, acc_i), (o_out, o_in)

    def rows_of(xi, c):
        return pl.ds(pl.multiple_of((xi * 2 + c) * 32, 32), 32)

    def pair_send(n):
        for xi in range(X):
            qt[n, xi] = accs[n][rows_of(xi, other), :].astype(BF16)
        put(pair[n], qt.at[n], rt.at[n], {"c": other})

    def x_send(n):
        arrived(pair[n])
        for off in (2, 1, 3):
            xi = at_off("x", off)
            v = accs[n][rows_of(xi, me["c"]), :] + rt[n, xi].astype(F32)
            uq[n, off - 1] = v.astype(BF16)
            put(b_x[n], uq.at[n, off - 1], rx.at[n, off - 1], {"x": xi})

    def x_fin(n):
        v = accs[n][rows_of(me["x"], me["c"]), :] + rt[n, me["x"]].astype(F32) + lora[n]
        arrived(b_x[n])
        for k in range(3):
            v = v + rx[n, k].astype(F32)
        res[n][...] = v.astype(BF16)

    def on_sub(fn):
        return lambda s: fn(bufs[s][8], SUBS[s][0], st[s])

    def on_half(fn):
        return lambda n: fn(halves["zy"[n]], "zy"[n], hst["zy"[n]])

    steps = {"gu": compute_gu, "hb": compute_hb, "sendgu": lambda s: rs1_send(s, slice(0, 2 * SUBS[s][2])),
             "sendhb": lambda s: rs1_send(s, slice(2 * SUBS[s][2], WIDTHS[s])), "agg": rs1_agg, "sum": rs1_fin,
             "mid": middle, "spread": on_sub(spread), "fwd": on_sub(forward),
             "fin": lambda s: arrived(st[s]["b"]), "hspread": on_half(spread), "hfwd": on_half(forward),
             "hfin": lambda n: arrived(hst["zy"[n]]["b"]),
             "out": post_o, "in": post_i, "flip": flip, "grad": grads, "hgrad": h_grads,
             "esend": e_send, "esum": e_sum, "emore": e_more, "efin": e_fin,
             "pair": pair_send, "xsend": x_send, "xfin": x_fin}
    for step, s in SCHEDULE:
        with jax.named_scope(step + str(s)):
            steps[step](s)
    pltpu.make_async_copy(bytes_of(SENT_TILES), bytes_of(SENT_TILES), send_sem).wait()
    assert (len(arrivals), moved[0]) == (N_RECV, SENT_TILES), (len(arrivals), moved[0])


RESULTS = (
    ((32, DS), BF16), ((32, DS), BF16), ((2, R, DS), F32),
    ((2, R, FS), F32), ((R, FS), F32), ((R, DS), F32),
)


def store(*refs):
    copies = [pltpu.make_async_copy(refs[n], refs[6 + n], refs[12].at[n]) for n in (3, 4, 2, 5, 0, 1)]
    for c in copies:
        c.start()
    for c in copies:
        c.wait()


def per_device(tok, w, wd, a, b, din, dout, cot):
    at = jnp.swapaxes(a, 1, 2).reshape(2 * R, DS)
    dint = jnp.swapaxes(din, 0, 1)
    vm = pltpu.VMEM
    scratch = [
        vm((2, X * C, 32, DS), BF16), vm((2, DS, FS), BF16), vm((FS, DS), BF16),
        vm((128, DS), BF16), vm((128, DS), BF16), vm((3, 128, FS), BF16),
        vm((T, DS), F32), vm((T, DS), F32),
        vm((16, EXT), BF16), vm((16, EXT), F32), vm((EXT, T), BF16), vm((2, 32, DS), F32),
        vm((2, X, 32, DS), BF16), vm((2, X, 32, DS), BF16),
        vm((2, 3, 32, DS), BF16), vm((2, 3, 32, DS), BF16),
        vm((16, EXT), BF16), vm((7, 16, EXT), BF16), vm((Y, Z, 16, EXT), BF16),
        vm((max(SENT_TILES, LOAD_TILES), 16, 128), BF16),
        vm((Y, Z, 16, HALVES["y"][2]), BF16), vm((Y, Z, 16, HALVES["z"][2]), BF16),
    ]
    for wid, (_, _, hw, _) in zip(WIDTHS, SUBS):
        scratch += [
            vm((Y, Z, 16, wid), F32), vm((Y, Z, 16, wid), BF16),
            vm((2, 2, 16, wid), BF16), vm((2, 2, 16, wid), BF16), vm((2, 4, 16, wid), BF16),
            vm((4, 16, wid), F32), vm((4, 16, wid), BF16), vm((3, 16, wid), BF16),
            vm((Y, Z, 16, 2 * hw), BF16),
        ]
    scratch += [pltpu.SemaphoreType.DMA((3,)), pltpu.SemaphoreType.DMA, pltpu.SemaphoreType.DMA((N_RECV,))]
    anyspec = pl.BlockSpec(memory_space=pltpu.MemorySpace.HBM)
    vspec = pl.BlockSpec(memory_space=pltpu.VMEM)
    res = pl.pallas_call(
        body,
        out_shape=tuple(vm(s, d) for s, d in RESULTS),
        in_specs=[anyspec] * 8,
        out_specs=(vspec,) * 6,
        scratch_shapes=scratch,
        compiler_params=pltpu.CompilerParams(
            collective_id=0, has_side_effects=True, vmem_limit_bytes=40 * 1024 * 1024),
        name="layer",
    )(*(pltpu.with_memory_space_constraint(v, pltpu.MemorySpace.HBM)
        for v in (tok, w, wd, at, b, dint, dout, cot)))
    out, inp, gl, gf, di, do = pl.pallas_call(
        store,
        out_shape=tuple(jax.ShapeDtypeStruct(s, d) for s, d in RESULTS),
        in_specs=[vspec] * 6,
        out_specs=(anyspec,) * 6,
        scratch_shapes=[pltpu.SemaphoreType.DMA((6,))],
        compiler_params=pltpu.CompilerParams(vmem_limit_bytes=1024 * 1024),
        name="store",
    )(*res)
    return out, inp, jnp.swapaxes(gl, 1, 2), gf, jnp.swapaxes(di, 0, 1), do


def solution(mesh):
    torus = Mesh(mesh.devices.reshape(X, C, Y, Z), ("x", "c", "y", "z"))
    dp, mp = ("x", "c"), ("y", "z")
    in_specs = (
        P(dp, mp), P(None, mp, dp), P(dp, mp), P(None, mp, None),
        P(None, None, dp), P(dp, None), P(None, mp), P(dp, mp),
    )
    out_specs = (P(dp, mp), P(dp, mp), P(None, mp, None), P(None, None, dp), P(dp, None), P(None, mp))
    return jax.shard_map(per_device, mesh=torus, in_specs=in_specs, out_specs=out_specs, check_vma=False)
```

```python
import math

import jax
import jax.numpy as jnp
from jax import lax
from jax.experimental import pallas as pl
from jax.experimental.pallas import tpu as pltpu
from jax.sharding import Mesh
from jax.sharding import PartitionSpec as P

MESH = pl.DeviceIdType.MESH
F32 = jnp.float32
BF16 = jnp.bfloat16

X, C, Y, Z = 4, 2, 4, 4
T = 256
DS = 512
FS = 1920
R = 64
EXT = 256
SCALE = 2.0 * T ** -0.5

SUBS = (
    ("z", 1024, 128, True), ("y", 0, 256, False), ("z", 1152, 256, False), ("y", 256, 256, False),
    ("z", 1408, 256, False), ("y", 512, 256, False), ("z", 1664, 256, False), ("y", 768, 256, False),
)
WIDTHS = tuple(3 * hw + (EXT if ext else 0) for _, _, hw, ext in SUBS)
HALVES = {"y": (0, 1024, 1024), "z": (1024, 896, 896 + EXT)}
NS = len(SUBS)
N_RECV = 17 + 4 * NS
TILE = 16 * 128
SENT_TILES = 30 * sum(WIDTHS) // 128 + 268
LOAD_TILES = (3 * R * DS + 3 * R * FS + 3 * DS * FS) // TILE


def steps_of(subs, *names):
    return [(name, s) for s in subs for name in names]


SCHEDULE = (
    [("gate", 1), ("sendgate", 1), ("gu", 0), ("sendgu", 0), ("up", 1), ("sendup", 1), ("gu", 2), ("sendgu", 2)]
    + steps_of((1, 0, 2), "hb", "sendhb")
    + steps_of(range(3, NS), "gu", "sendgu", "hb", "sendhb")
    + steps_of(range(NS), "agg") + steps_of(range(NS), "sum") + steps_of(range(NS), "mid")
    + [("esend", 0)] + steps_of(range(4), "spread") + steps_of(range(2), "hspread") + steps_of(range(4, 6), "spread")
    + steps_of(range(2), "hfwd") + steps_of(range(6, NS), "spread") + steps_of(range(4), "fwd")
    + [("esum", 0)] + steps_of(range(4, 6), "fwd")
    + [("hfin", 0), ("hfin", 1)] + steps_of(range(6, NS), "fwd") + [("out", 0), ("pair", 0)]
    + steps_of(range(2), "fin", "in") + [("xsend", 0)]
    + steps_of(range(2, 4), "fin", "in") + [("emore", 0)]
    + steps_of(range(4, NS), "fin", "in") + [("pair", 1), ("flip", 0), ("hgrad", 0)]
    + steps_of(range(3), "grad") + [("xsend", 1)] + steps_of(range(3, NS), "grad")
    + [("efin", 0), ("xfin", 0), ("xfin", 1)]
)


def nn(a, b):
    return jnp.dot(a, b, preferred_element_type=F32)


def nt(a, b):
    return lax.dot_general(a, b, (((1,), (1,)), ((), ())), preferred_element_type=F32)


def body(tok, w_hbm, wd_hbm, at_hbm, b_hbm, dint_hbm, dout_hbm, cot,
         o_out, o_in, o_gl, o_gf, o_di, o_do,
         xc, w, wd, aw, cw, ew, acc_o, acc_i, ext2, e_acc, ext_t, lora,
         qt, rt, uq, rx, e_out, e_in, eg, bytes_ref, h_y, h_z, *rest):
    per = len(rest) - 3
    each = per // NS
    bufs = [rest[s * each:(s + 1) * each] for s in range(NS)]
    local_sem, send_sem, recv_sem = rest[per:]
    me = {a: lax.axis_index(a) for a in ("x", "c", "y", "z")}

    def at_off(axis, off):
        return lax.rem(me[axis] + off, 4)

    arrivals, moved = [], [0]

    def bytes_of(tiles):
        return bytes_ref.at[0:tiles]

    def group(like, same=None):
        if same is not None:
            return same[0], like
        arrivals.append(like)
        return len(arrivals) - 1, like

    def put(g, src, dst, device):
        moved[0] += math.prod(src.shape) // TILE
        pltpu.make_async_remote_copy(
            src_ref=src, dst_ref=dst, send_sem=send_sem, recv_sem=recv_sem.at[g[0]],
            device_id=device, device_id_type=MESH).start()

    def arrived(g):
        size = bytes_of(g[1])
        pltpu.make_async_copy(size, size, recv_sem.at[g[0]]).wait()

    other = 1 - me["c"]
    barrier = pltpu.get_barrier_semaphore()
    partners = [{"c": other}]
    for off in (1, 2, 3):
        partners += [{"x": at_off("x", off)}, {"x": at_off("x", off), "c": other},
                     {"y": at_off("y", off)}, {"z": at_off("z", off)}]
    for p in partners:
        pl.semaphore_signal(barrier, inc=1, device_id=p, device_id_type=MESH)

    my_dp = me["x"] * 2 + me["c"]
    loads = []
    for n, (src, dst) in enumerate(((tok, xc.at[0, my_dp]), (cot, xc.at[1, my_dp]))):
        loads.append(pltpu.make_async_copy(src, dst, local_sem.at[n]))
        loads[n].start()
    for src, dst in (
        (at_hbm, aw), (dout_hbm, cw.at[0:64]), (b_hbm.at[0], ew.at[0, 0:64]), (b_hbm.at[1], ew.at[1, 64:128]),
        (dint_hbm, ew.at[2, 0:64]), (w_hbm, w), (wd_hbm, wd),
    ):
        pltpu.make_async_copy(src, dst, local_sem.at[2]).start()
    cw[64:128, :] = jnp.zeros((64, DS), BF16)
    ew[0, 64:128, :] = jnp.zeros((64, FS), BF16)
    ew[1, 0:64, :] = jnp.zeros((64, FS), BF16)
    ew[2, 64:128, :] = jnp.zeros((64, FS), BF16)
    loads[0].wait()
    loads[1].wait()
    pl.semaphore_wait(barrier, len(partners))

    def block(n, off):
        return xc.at[n, at_off("x", off) * 2 + me["c"]]

    along = [group(3 * 8) for _ in range(2)]
    across = [group(4 * 8) for _ in range(2)]
    for n in range(2):
        for off in (2, 1, 3):
            put(along[n], block(n, 0), block(n, 0), {"x": at_off("x", off)})
        put(across[n], block(n, 0), block(n, 0), {"c": other})
    pltpu.make_async_copy(bytes_of(LOAD_TILES), bytes_of(LOAD_TILES), local_sem.at[2]).wait()
    for n in range(2):
        arrived(along[n])
        for off in (1, 2, 3):
            put(across[n], block(n, off), block(n, off), {"c": other})

    arrived(across[0])
    seen = set()

    def rows_all(n):
        return xc[n].reshape(T, DS)

    def seg(n, hw):
        return slice(n * hw, (n + 1) * hw)

    def keep(s, cols, v):
        v = v.reshape(Y, Z, 16, v.shape[-1])
        bufs[s][0][:, :, :, cols] = v
        bufs[s][1][:, :, :, cols] = v.astype(BF16)

    def compute_gu(s, which=(0, 1)):
        _, f0, hw, _ = SUBS[s]
        cols = slice(f0, f0 + hw)
        for n in which:
            keep(s, seg(n, hw), nn(rows_all(0), w[n, :, cols]))

    def compute_hb(s):
        _, f0, hw, ext = SUBS[s]
        cols = slice(f0, f0 + hw)
        if "cot" not in seen:
            arrived(across[1])
            seen.add("cot")
        keep(s, seg(2, hw), nt(rows_all(1), wd[cols, :]))
        if ext:
            keep(s, slice(3 * hw, 3 * hw + 128), nt(rows_all(0), aw[...]))
            keep(s, slice(3 * hw + 128, 3 * hw + EXT), nt(rows_all(1), cw[...]))

    other_axis = {"y": "z", "z": "y"}

    def part(ref, a, a1, lo, hi, cols=slice(None)):
        if a == "y":
            return ref.at[a1, lo:hi, :, cols]
        return ref.at[lo:hi, a1, :, cols]

    def value(ref, s, a1, a2):
        if SUBS[s][0] == "y":
            return ref[a1, a2]
        return ref[a2, a1]

    st = []
    for s in range(NS):
        n, g = WIDTHS[s] // 128, 2 * SUBS[s][2] // 128
        t, f = group(4 * n), group(8 * n)
        st.append({"t": t, "f": f, "r": group(3 * n), "a": group(3 * g, f),
                   "t2": group(4 * g, t), "b": group(8 * g)})

    halves = {"y": h_y, "z": h_z}
    hst = {}
    for a, (_, _, n) in HALVES.items():
        hst[a] = {"a": group(3 * n // 128), "t2": group(4 * n // 128), "b": group(8 * n // 128)}

    def ring(s):
        a = SUBS[s][0]
        return a, {a: at_off(a, 3)}, {a: at_off(a, 1)}

    def rs1_send(s, cols):
        a, left, right = ring(s)
        q, tt, ff = bufs[s][1], bufs[s][2], bufs[s][4]
        put(st[s]["t"], part(q, a, at_off(a, 2), 0, 2, cols), tt.at[0, :, :, cols], left)
        put(st[s]["t"], part(q, a, at_off(a, 2), 2, 4, cols), tt.at[1, :, :, cols], right)
        put(st[s]["f"], part(q, a, at_off(a, 3), 2, 4, cols), ff.at[0, 2:4, :, cols], left)
        put(st[s]["f"], part(q, a, at_off(a, 1), 0, 2, cols), ff.at[1, 0:2, :, cols], right)

    def rs1_agg(s):
        a, left, right = ring(s)
        p, tt, gg, ff = bufs[s][0], bufs[s][2], bufs[s][3], bufs[s][4]
        arrived(st[s]["t"])
        for j in range(2):
            gg[0, j] = (value(p, s, at_off(a, 3), j) + tt[0, j].astype(F32)).astype(BF16)
        put(st[s]["f"], gg.at[0], ff.at[0, 0:2], left)
        for j in range(2):
            gg[1, j] = (value(p, s, at_off(a, 1), 2 + j) + tt[1, j].astype(F32)).astype(BF16)
        put(st[s]["f"], gg.at[1], ff.at[1, 2:4], right)

    def rs1_fin(s):
        a = SUBS[s][0]
        b = other_axis[a]
        p, ff, sm, q2, r2 = (bufs[s][k] for k in (0, 4, 5, 6, 7))
        arrived(st[s]["f"])
        for j in range(4):
            v = value(p, s, me[a], j) + ff[0, j].astype(F32) + ff[1, j].astype(F32)
            sm[j] = v
            q2[j] = v.astype(BF16)
        for off in (2, 1, 3):
            put(st[s]["r"], q2.at[at_off(b, off)], r2.at[off - 1], {b: at_off(b, off)})

    def add(ref, key, v):
        if key in seen:
            v = v + ref[...]
        seen.add(key)
        ref[...] = v

    def middle(s):
        a, f0, hw, ext = SUBS[s]
        b = other_axis[a]
        sm, r2, act = (bufs[s][k] for k in (5, 7, 8))
        hid_ref, h0 = halves[a], f0 - HALVES[a][0]
        arrived(st[s]["r"])

        def total(cols):
            v = sm[me[b], :, cols]
            for n in range(3):
                v = v + r2[n, :, cols].astype(F32)
            return v

        my = (me["y"], me["z"])
        cols = slice(f0, f0 + hw)
        if ext:
            v = total(slice(3 * hw, 3 * hw + EXT)).astype(BF16)
            hid_ref[my[0], my[1], :, HALVES[a][1]:] = v
            ext2[...] = 2.0 * v
        lows = (ext2[:, 0:128], ext2[:, 0:128], ext2[:, 128:256])
        gate, up, hb = (total(seg(n, hw)) + nn(lows[n], ew[n, :, cols]) for n in range(3))
        sg = 1.0 / (1.0 + jnp.exp(-gate))
        gs = gate * sg
        hid = (gs * up).astype(BF16)
        gb = (hb * up * sg * (1.0 + gate * (1.0 - sg))).astype(BF16)
        ub = (hb * gs).astype(BF16)
        hid_ref[my[0], my[1], :, h0:h0 + hw] = hid
        act[my[0], my[1], :, seg(0, hw)] = gb
        act[my[0], my[1], :, seg(1, hw)] = ub
        pieces = [slice(h0, h0 + hw)] + ([slice(HALVES[a][1], HALVES[a][1] + EXT)] if ext else [])
        for piece in pieces:
            mine = hid_ref.at[my[0], my[1], :, piece]
            for off in (2, 1, 3):
                put(hst[a]["a"], mine, mine, {b: at_off(b, off)})
        near(s)
        add(e_acc.at[:, 0:128], "bl", nt(gb, ew[0, :, cols]) + nt(ub, ew[1, :, cols]))
        add(e_acc.at[:, 128:256], "ld", nt(hid, ew[2, :, cols]))

    def near(s):
        b, mine = other_axis[SUBS[s][0]], bufs[s][8].at[me["y"], me["z"]]
        for off in (2, 1, 3):
            put(st[s]["a"], mine, mine, {b: at_off(b, off)})

    def spread(ref, a, groups):
        left, right = {a: at_off(a, 3)}, {a: at_off(a, 1)}
        arrived(groups["a"])
        lo, hi = part(ref, a, me[a], 0, 2), part(ref, a, me[a], 2, 4)
        put(groups["t2"], lo, lo, left)
        put(groups["t2"], hi, hi, right)
        put(groups["b"], hi, hi, left)
        put(groups["b"], lo, lo, right)

    def forward(ref, a, groups):
        left, right = {a: at_off(a, 3)}, {a: at_off(a, 1)}
        arrived(groups["t2"])
        src = part(ref, a, at_off(a, 1), 0, 2)
        put(groups["b"], src, src, left)
        src = part(ref, a, at_off(a, 3), 2, 4)
        put(groups["b"], src, src, right)

    def all_rows(ref, cols):
        return ref[:, :, :, cols].reshape(T, cols.stop - cols.start)

    def post_o(_):
        v = [nn(all_rows(halves[a], slice(0, n)), wd[f0:f0 + n, :]) for a, (f0, n, _) in HALVES.items()]
        acc_o[...] = v[0] + v[1]

    def post_i(s):
        _, f0, hw, _ = SUBS[s]
        cols = slice(f0, f0 + hw)
        act = bufs[s][8]
        add(acc_i, "i", nt(all_rows(act, seg(0, hw)), w[0, :, cols]) + nt(all_rows(act, seg(1, hw)), w[1, :, cols]))

    def flip(_):
        n = HALVES["z"][1]
        ext_t[...] = jnp.transpose(all_rows(h_z, slice(n, n + EXT)).astype(F32)).astype(BF16)

    def h_grads(_):
        for a, (f0, n, _) in HALVES.items():
            o_di[:, f0:f0 + n] = SCALE * nn(ext_t[128:192, :], all_rows(halves[a], slice(0, n)))

    def grads(s):
        _, f0, hw, _ = SUBS[s]
        cols = slice(f0, f0 + hw)
        for k in range(2):
            o_gf[k, :, cols] = SCALE * nn(ext_t[64 * k:64 * k + 64, :], all_rows(bufs[s][8], seg(k, hw)))

    my_rows = (me["y"], me["z"])
    e_dp, e_z, e_y = group(7 * 2), group(3 * 2), group(12 * 2)
    hops = [(off, d) for off in (2, 1, 3, 0) for d in (0, 1) if off or d]

    def e_send(_):
        e_out[...] = e_acc[...].astype(BF16)
        for n, (off, d) in enumerate(hops):
            put(e_dp, e_out, e_in.at[n], {"x": at_off("x", off), "c": lax.rem(me["c"] + d, 2)})

    def e_sum(_):
        arrived(e_dp)
        v = e_acc[...]
        for n in range(7):
            v = v + e_in[n].astype(F32)
        eg[my_rows[0], my_rows[1]] = v.astype(BF16)
        mine = eg.at[my_rows[0], my_rows[1]]
        for off in (2, 1, 3):
            put(e_z, mine, mine, {"z": at_off("z", off)})

    def e_more(_):
        arrived(e_z)
        mine = eg.at[my_rows[0]]
        for off in (2, 1, 3):
            put(e_y, mine, mine, {"y": at_off("y", off)})

    def e_fin(_):
        arrived(e_y)
        e_t = jnp.transpose(eg[...].reshape(T, EXT).astype(F32)).astype(BF16)
        for k in range(2):
            o_gl[k] = SCALE * nn(e_t[64 * k:64 * k + 64], xc[0].reshape(T, DS))
        o_do[...] = SCALE * nn(e_t[128:192], xc[1].reshape(T, DS))
        e2 = 2.0 * eg[me["x"], pl.ds(2 * me["c"], 2)].reshape(32, EXT)
        lora[0] = nn(e2[:, 128:256], cw[...])
        lora[1] = nn(e2[:, 0:128], aw[...])

    pair = [group(4 * 8) for n in range(2)]
    b_x = [group(3 * 8) for n in range(2)]
    accs, res = (acc_o, acc_i), (o_out, o_in)

    def rows_of(xi, c):
        return pl.ds(pl.multiple_of((xi * 2 + c) * 32, 32), 32)

    def pair_send(n):
        for xi in range(X):
            qt[n, xi] = accs[n][rows_of(xi, other), :].astype(BF16)
        put(pair[n], qt.at[n], rt.at[n], {"c": other})

    def x_send(n):
        arrived(pair[n])
        for off in (2, 1, 3):
            xi = at_off("x", off)
            v = accs[n][rows_of(xi, me["c"]), :] + rt[n, xi].astype(F32)
            uq[n, off - 1] = v.astype(BF16)
            put(b_x[n], uq.at[n, off - 1], rx.at[n, off - 1], {"x": xi})

    def x_fin(n):
        v = accs[n][rows_of(me["x"], me["c"]), :] + rt[n, me["x"]].astype(F32) + lora[n]
        arrived(b_x[n])
        for k in range(3):
            v = v + rx[n, k].astype(F32)
        res[n][...] = v.astype(BF16)

    def on_sub(fn):
        return lambda s: fn(bufs[s][8], SUBS[s][0], st[s])

    def on_half(fn):
        return lambda n: fn(halves["zy"[n]], "zy"[n], hst["zy"[n]])

    steps = {"gate": lambda s: compute_gu(s, (0,)), "up": lambda s: compute_gu(s, (1,)),
             "sendgate": lambda s: rs1_send(s, seg(0, SUBS[s][2])), "sendup": lambda s: rs1_send(s, seg(1, SUBS[s][2])),
             "gu": compute_gu, "hb": compute_hb, "sendgu": lambda s: rs1_send(s, slice(0, 2 * SUBS[s][2])),
             "sendhb": lambda s: rs1_send(s, slice(2 * SUBS[s][2], WIDTHS[s])), "agg": rs1_agg, "sum": rs1_fin,
             "mid": middle, "spread": on_sub(spread), "fwd": on_sub(forward),
             "fin": lambda s: arrived(st[s]["b"]), "hspread": on_half(spread), "hfwd": on_half(forward),
             "hfin": lambda n: arrived(hst["zy"[n]]["b"]),
             "out": post_o, "in": post_i, "flip": flip, "grad": grads, "hgrad": h_grads,
             "esend": e_send, "esum": e_sum, "emore": e_more, "efin": e_fin,
             "pair": pair_send, "xsend": x_send, "xfin": x_fin}
    for step, s in SCHEDULE:
        with jax.named_scope(step + str(s)):
            steps[step](s)
    pltpu.make_async_copy(bytes_of(SENT_TILES), bytes_of(SENT_TILES), send_sem).wait()
    assert (len(arrivals), moved[0]) == (N_RECV, SENT_TILES), (len(arrivals), moved[0])


RESULTS = (
    ((32, DS), BF16), ((32, DS), BF16), ((2, R, DS), F32),
    ((2, R, FS), F32), ((R, FS), F32), ((R, DS), F32),
)


def store(*refs):
    copies = [pltpu.make_async_copy(refs[n], refs[6 + n], refs[12].at[n]) for n in (3, 4, 2, 5, 0, 1)]
    for c in copies:
        c.start()
    for c in copies:
        c.wait()


def per_device(tok, w, wd, a, b, din, dout, cot):
    at = jnp.swapaxes(a, 1, 2).reshape(2 * R, DS)
    dint = jnp.swapaxes(din, 0, 1)
    vm = pltpu.VMEM
    scratch = [
        vm((2, X * C, 32, DS), BF16), vm((2, DS, FS), BF16), vm((FS, DS), BF16),
        vm((128, DS), BF16), vm((128, DS), BF16), vm((3, 128, FS), BF16),
        vm((T, DS), F32), vm((T, DS), F32),
        vm((16, EXT), BF16), vm((16, EXT), F32), vm((EXT, T), BF16), vm((2, 32, DS), F32),
        vm((2, X, 32, DS), BF16), vm((2, X, 32, DS), BF16),
        vm((2, 3, 32, DS), BF16), vm((2, 3, 32, DS), BF16),
        vm((16, EXT), BF16), vm((7, 16, EXT), BF16), vm((Y, Z, 16, EXT), BF16),
        vm((max(SENT_TILES, LOAD_TILES), 16, 128), BF16),
        vm((Y, Z, 16, HALVES["y"][2]), BF16), vm((Y, Z, 16, HALVES["z"][2]), BF16),
    ]
    for wid, (_, _, hw, _) in zip(WIDTHS, SUBS):
        scratch += [
            vm((Y, Z, 16, wid), F32), vm((Y, Z, 16, wid), BF16),
            vm((2, 2, 16, wid), BF16), vm((2, 2, 16, wid), BF16), vm((2, 4, 16, wid), BF16),
            vm((4, 16, wid), F32), vm((4, 16, wid), BF16), vm((3, 16, wid), BF16),
            vm((Y, Z, 16, 2 * hw), BF16),
        ]
    scratch += [pltpu.SemaphoreType.DMA((3,)), pltpu.SemaphoreType.DMA, pltpu.SemaphoreType.DMA((N_RECV,))]
    anyspec = pl.BlockSpec(memory_space=pltpu.MemorySpace.HBM)
    vspec = pl.BlockSpec(memory_space=pltpu.VMEM)
    res = pl.pallas_call(
        body,
        out_shape=tuple(vm(s, d) for s, d in RESULTS),
        in_specs=[anyspec] * 8,
        out_specs=(vspec,) * 6,
        scratch_shapes=scratch,
        compiler_params=pltpu.CompilerParams(
            collective_id=0, has_side_effects=True, vmem_limit_bytes=40 * 1024 * 1024),
        name="layer",
    )(*(pltpu.with_memory_space_constraint(v, pltpu.MemorySpace.HBM)
        for v in (tok, w, wd, at, b, dint, dout, cot)))
    out, inp, gl, gf, di, do = pl.pallas_call(
        store,
        out_shape=tuple(jax.ShapeDtypeStruct(s, d) for s, d in RESULTS),
        in_specs=[vspec] * 6,
        out_specs=(anyspec,) * 6,
        scratch_shapes=[pltpu.SemaphoreType.DMA((6,))],
        compiler_params=pltpu.CompilerParams(vmem_limit_bytes=1024 * 1024),
        name="store",
    )(*res)
    return out, inp, jnp.swapaxes(gl, 1, 2), gf, jnp.swapaxes(di, 0, 1), do


def solution(mesh):
    torus = Mesh(mesh.devices.reshape(X, C, Y, Z), ("x", "c", "y", "z"))
    dp, mp = ("x", "c"), ("y", "z")
    in_specs = (
        P(dp, mp), P(None, mp, dp), P(dp, mp), P(None, mp, None),
        P(None, None, dp), P(dp, None), P(None, mp), P(dp, mp),
    )
    out_specs = (P(dp, mp), P(dp, mp), P(None, mp, None), P(None, None, dp), P(dp, None), P(None, mp))
    return jax.shard_map(per_device, mesh=torus, in_specs=in_specs, out_specs=out_specs, check_vma=False)
```
